256 devices in a mesh: radial: 64 (over x, z, core), phi: 4 (over y).
Axes of the slice: x: 4, y: 4, z: 8, core: 2. Of those that a mesh axis runs over, the one named last changes fastest.
Arguments:
- conserved: float32 [8, 512, 64, 128], P(None, 'radial', 'phi'), may hold values from -2.5 to 7, as said below
- core_mass: float32 [1], replicated, may hold values from 0.2 to 1
Outputs:
- advanced: float32 [8, 512, 64, 128], P(None, 'radial', 'phi')
- enclosed_mass: float32 [512], P('radial')
The draws below stay inside these ranges and needn't reach their ends.
Inputs may be any that keep to these rules, and one draw needn't show every extreme that they name: conserved[0] (density) lies between 0.4 and 2.5; conserved[4] exceeds (conserved[1]^2 + conserved[2]^2 + conserved[3]^2)/(2 conserved[0]) by at least 0.6; the speeds |conserved[m]/conserved[0]| stay below 1; conserved[5..7] lie between 0 and conserved[0].
All inputs are finite; a program needn't handle non-finite values.
Results may differ from the reference program's by a relative error of at most 0.0003.
Values sent between devices are 32-bit elements; how exact they have to be, the bound alone decides.
A program may use at most 64 MiB of HBM per device.

```python
import math
import jax
import jax.numpy as jnp
from jax import lax

RD = 8
NT = 128
NR = 512
NP = 64


def draw_conserved(key, part):
    subkeys = jax.random.split(key, 12)
    shape = (NR, NP, NT)
    depth = (jnp.arange(NR, dtype=jnp.float32) + 0.5) / NR
    azimuth = (jnp.arange(NP, dtype=jnp.float32) + 0.5) * (2.0 * math.pi / NP)
    centres = jax.random.uniform(subkeys[6], (3,), jnp.float32, 0.0, 1.0)
    heights = jax.random.uniform(subkeys[7], (3,), jnp.float32, -0.13, 0.13)
    bumps = jnp.exp(-jnp.square((depth[:, None] - centres[None, :]) / 0.15))
    profile = jnp.exp(jnp.sum(bumps * heights[None, :], axis=1))
    turn = jax.random.uniform(subkeys[8], (), jnp.float32, 0.0, 2.0 * math.pi)
    twist = jax.random.uniform(subkeys[9], (), jnp.float32, -0.5 * math.pi, 0.5 * math.pi)
    phase = turn + twist * depth
    angular = 1.0 + 0.35 * jnp.cos(azimuth[None, :] - phase[:, None])
    smooth = (profile[:, None] * angular)[:, :, None]
    rough = jnp.exp(jax.random.uniform(subkeys[0], shape, jnp.float32, jnp.log(0.75), jnp.log(1.33)))
    density = jnp.clip(smooth * rough, 0.4, 2.5)
    speeds = [jnp.clip(0.3 * jax.random.normal(subkeys[1 + which], shape, jnp.float32), -0.99, 0.99) for which in range(3)]
    pressure = jax.random.uniform(subkeys[4], shape, jnp.float32, 0.3, 0.9)
    kinetic = 0.5 * density * (speeds[0] * speeds[0] + speeds[1] * speeds[1] + speeds[2] * speeds[2])
    energy = pressure / (4.0 / 3.0 - 1.0) + kinetic
    tracers = jax.random.uniform(subkeys[5], (3,) + shape, jnp.float32, 0.0, 1.0) * density[None]
    momenta = jnp.stack([density * speeds[0], density * speeds[1], density * speeds[2]])
    return jnp.concatenate([density[None], momenta, energy[None], tracers], axis=0)


def setup_inputs(seed: int = 0) -> dict:
    streams_of = jax.random.split(jax.random.key(seed), 3)
    conserved = draw_conserved(jax.random.fold_in(streams_of[2], 71), 0)
    core_mass = jnp.clip(jnp.exp(jax.random.uniform(streams_of[1], (1,), jnp.float32, math.log(0.2), math.log(1.0))), 0.2, 1.0)
    return {"conserved": conserved, "core_mass": core_mass}


ADIABATIC = 4.0 / 3.0
INNER_RADIUS = 1.0
OUTER_RADIUS = 2.0
COURANT = 0.4
GRAVITY_KICK = 0.004
MINIMUM_DENSITY = 0.05
PRESSURE_FLOOR = 0.01

def step_sizes(radial_total, phi_total, theta_total):
    theta_step = math.pi / theta_total
    phi_step = 2.0 * math.pi / phi_total
    polar_width = INNER_RADIUS * math.sin(0.5 * theta_step) * phi_step
    radial_step = min(2.0 * polar_width, (OUTER_RADIUS - INNER_RADIUS) / radial_total)
    timestep = COURANT * min(radial_step, polar_width)
    return (radial_step, theta_step, phi_step, timestep)

def thermo(values):
    density = jnp.maximum(values[0], MINIMUM_DENSITY)
    kinetic = 0.5 * (values[1] * values[1] + values[2] * values[2] + values[3] * values[3]) / density
    pressure = jnp.maximum((ADIABATIC - 1.0) * (values[4] - kinetic), PRESSURE_FLOOR * density)
    return (density, pressure)

def physical(values, component):
    density, pressure = thermo(values)
    normal = values[component] / density
    sound = jnp.sqrt(ADIABATIC * pressure / density)
    pieces = [values[which] * normal for which in range(values.shape[0])]
    pieces[component] = pieces[component] + pressure
    pieces[4] = pieces[4] + pressure * normal
    return (jnp.stack(pieces), jnp.abs(normal) + sound)

def face_flux(values, along_dim, component):
    interior = values.shape[along_dim] - 4
    neighbour_differences = lax.slice_in_dim(values, 1, interior + 4, axis=along_dim) - lax.slice_in_dim(values, 0, interior + 3, axis=along_dim)
    below_diff = lax.slice_in_dim(neighbour_differences, 0, interior + 2, axis=along_dim)
    above_diff = lax.slice_in_dim(neighbour_differences, 1, interior + 3, axis=along_dim)
    limited = 0.5 * (jnp.sign(below_diff) + jnp.sign(above_diff)) * jnp.minimum(jnp.abs(below_diff), jnp.abs(above_diff))
    left_state = lax.slice_in_dim(values, 1, interior + 2, axis=along_dim) + 0.5 * lax.slice_in_dim(limited, 0, interior + 1, axis=along_dim)
    right_state = lax.slice_in_dim(values, 2, interior + 3, axis=along_dim) - 0.5 * lax.slice_in_dim(limited, 1, interior + 2, axis=along_dim)
    left_flux, left_signal = physical(left_state, component)
    right_flux, right_signal = physical(right_state, component)
    signal = jnp.maximum(left_signal, right_signal)
    return 0.5 * (left_flux + right_flux) - 0.5 * signal * (right_state - left_state)

def hydro_rate(extended, cell_centers, enclosed, radial_step, theta_step, phi_step, strength):
    theta_cells = extended.shape[3]
    centre_cells = extended[:, 2:-2, 2:-2, :]
    polar_padded = jnp.pad(centre_cells, ((0, 0), (0, 0), (0, 0), (2, 2)), mode='edge')
    radial_flux = face_flux(extended[:, :, 2:-2, :], 1, 1)
    polar_flux = face_flux(polar_padded, 3, 2)
    azimuth_flux = face_flux(extended[:, 2:-2, :, :], 2, 3)
    angles = (jnp.arange(theta_cells, dtype=jnp.float32) + 0.5) * theta_step
    sine_center = jnp.sin(angles)
    cosine = jnp.cos(angles)
    face_sine = jnp.sin(jnp.arange(theta_cells + 1, dtype=jnp.float32) * theta_step)
    radius = cell_centers[:, None, None]
    face_radius = jnp.concatenate([cell_centers - 0.5 * radial_step, cell_centers[-1:] + 0.5 * radial_step])[:, None, None]
    radial_area = face_radius * face_radius * radial_flux
    divergence = (radial_area[:, 1:] - radial_area[:, :-1]) / (radius * radius * radial_step)
    polar_area = face_sine * polar_flux
    divergence = divergence + (polar_area[..., 1:] - polar_area[..., :-1]) / (radius * sine_center * theta_step)
    divergence = divergence + (azimuth_flux[:, :, 1:] - azimuth_flux[:, :, :-1]) / (radius * sine_center * phi_step)
    density, pressure = thermo(centre_cells)
    radial_speed = centre_cells[1] / density
    polar_speed = centre_cells[2] / density
    azimuth_speed = centre_cells[3] / density
    cotangent = cosine / sine_center
    gravity_pull = strength * enclosed[:, None, None] / (radius * radius)
    source_radial = (2.0 * pressure + density * (polar_speed * polar_speed + azimuth_speed * azimuth_speed)) / radius - density * gravity_pull
    source_polar = (pressure * cotangent + density * azimuth_speed * azimuth_speed * cotangent - density * radial_speed * polar_speed) / radius
    source_azimuth = -density * azimuth_speed * (radial_speed + polar_speed * cotangent) / radius
    source_energy = -centre_cells[1] * gravity_pull
    nothing = jnp.zeros_like(pressure)
    source = jnp.stack([nothing, source_radial, source_polar, source_azimuth, source_energy, nothing, nothing, nothing])
    return source - divergence

def reference(conserved, core_mass):
    radial_total = conserved.shape[1]
    phi_total = conserved.shape[2]
    theta_total = conserved.shape[3]
    radial_step, theta_step, phi_step, timestep = step_sizes(radial_total, phi_total, theta_total)
    strength = GRAVITY_KICK / timestep
    cell_centers = INNER_RADIUS + (jnp.arange(radial_total, dtype=jnp.float32) + 0.5) * radial_step
    sine_center = jnp.sin((jnp.arange(theta_total, dtype=jnp.float32) + 0.5) * theta_step)
    shells = jnp.dot(lax.optimization_barrier(jnp.sum(conserved[0], axis=1)), sine_center, precision=lax.Precision.HIGHEST)
    shells = shells * cell_centers * cell_centers * (radial_step * theta_step * phi_step)
    enclosed = core_mass[0] + jnp.cumsum(shells) - 0.5 * shells
    blocks = radial_total // RD

    def full_rate(values):
        padded = jnp.pad(values, ((0, 0), (2, 2), (0, 0), (0, 0)), mode='edge')
        padded = jnp.pad(padded, ((0, 0), (0, 0), (2, 2), (0, 0)), mode='wrap')

        def one_block(block_index):
            first_row = (block_index * RD).astype(jnp.int32)
            radial_segment = lax.dynamic_slice_in_dim(padded, first_row, RD + 4, 1)
            radius_part = lax.dynamic_slice_in_dim(cell_centers, first_row, RD, 0)
            mass_part = lax.dynamic_slice_in_dim(enclosed, first_row, RD, 0)
            return hydro_rate(radial_segment, radius_part, mass_part, radial_step, theta_step, phi_step, strength)
        stacked = lax.map(one_block, jnp.arange(blocks, dtype=jnp.int32))
        return jnp.transpose(stacked, (1, 0, 2, 3, 4)).reshape(values.shape)
    section_one = conserved + timestep * full_rate(conserved)
    section_two = section_one + timestep * full_rate(section_one)
    advanced = 0.5 * conserved + 0.5 * section_two
    return (advanced, enclosed)
```

```python
import math

import jax
import jax.numpy as jnp
import numpy as np
from jax import lax
from jax.experimental import pallas as pl
from jax.experimental.pallas import tpu as pltpu
from jax.sharding import PartitionSpec as P

ADIABATIC = 4.0 / 3.0
INNER_RADIUS = 1.0
OUTER_RADIUS = 2.0
COURANT = 0.4
GRAVITY_KICK = 0.004
MINIMUM_DENSITY = 0.05
PRESSURE_FLOOR = 0.01

MESH = pl.DeviceIdType.MESH
NV = 8
RD = 8
NW = 16
NT = 128
PAD = 8
ROWS = 32
XN, ZC, YN = 4, 16, 4
RADIAL = XN * ZC


def step_sizes(radial_total, phi_total, theta_total):
    theta_step = math.pi / theta_total
    phi_step = 2.0 * math.pi / phi_total
    polar_width = INNER_RADIUS * math.sin(0.5 * theta_step) * phi_step
    radial_step = min(2.0 * polar_width, (OUTER_RADIUS - INNER_RADIUS) / radial_total)
    timestep = COURANT * min(radial_step, polar_width)
    return (radial_step, theta_step, phi_step, timestep)


DR, DTH, DPH, DT = step_sizes(RADIAL * RD, YN * NW, NT)
STRENGTH = GRAVITY_KICK / DT


def polar_table():
    center = (np.arange(NT) + 0.5) * DTH
    face = np.arange(NT + 1) * DTH
    sine, face_sine = np.sin(center), np.sin(face)
    table = np.zeros((8, NT))
    table[0] = 0.5 * DT * face_sine[:-1] / (sine * DTH)
    table[1] = 0.5 * DT * face_sine[1:] / (sine * DTH)
    table[2] = 0.5 * DT / (sine * DPH)
    table[3] = np.cos(center) / sine
    table[4] = sine * (DR * DTH * DPH)
    return table.astype(np.float32)


def thermo(u):
    density = jnp.maximum(u[0], MINIMUM_DENSITY)
    inverse = 1.0 / density
    kinetic = 0.5 * (u[1] * u[1] + u[2] * u[2] + u[3] * u[3]) * inverse
    pressure = jnp.maximum((ADIABATIC - 1.0) * (u[4] - kinetic), PRESSURE_FLOOR * density)
    return density, inverse, pressure


def side(u, m):
    _, inverse, pressure = thermo(u)
    normal = u[m] * inverse
    square = ADIABATIC * pressure * inverse
    return pressure, normal, jnp.abs(normal) + square * lax.rsqrt(square)


def minmod(a, b):
    return jnp.maximum(jnp.minimum(a, b), jnp.minimum(jnp.maximum(a, b), 0.0))


def twice_flux(left, right, m):
    pl_, vl, al = side(left, m)
    pr_, vr, ar = side(right, m)
    signal = jnp.maximum(al, ar)
    cl, cr = vl + signal, vr - signal
    flux = [cl * a + cr * b for a, b in zip(left, right)]
    flux[m] = flux[m] + (pl_ + pr_)
    flux[4] = flux[4] + (pl_ * vl + pr_ * vr)
    return flux


def kernel(
    x_ref, core_ref, polar_ref, out_ref, enc_ref,
    e0, e1, acc, fp, out_v, tb, gt, enc_v, rows_src, rows_in, l1_in, l2_src, l2_in,
    load_sem, out_sem, enc_sem, h_send, h_recv, r_send, r_recv, a_send, a_recv, b_send, b_recv,
):
    r, y = lax.axis_index("radial"), lax.axis_index("phi")
    zc, xi = lax.rem(r, ZC), r // ZC
    first, last = r == 0, r == RADIAL - 1

    load = pltpu.make_async_copy(x_ref, e0.at[:, 2 : 2 + RD, PAD : PAD + NW, :], load_sem)
    load.start()

    line = [(xi * ZC + lax.rem(zc + d, ZC), y) for d in range(1, ZC)]
    wedge = [(r, lax.rem(y + d, YN)) for d in range(1, YN)]
    barrier = pltpu.get_barrier_semaphore()

    def greet(device):
        pl.semaphore_signal(barrier, inc=1, device_id=device, device_id_type=MESH)

    for device in line + wedge:
        greet(device)
    for d in range(1, XN):

        @pl.when(xi - d >= 0)
        def _(d=d):
            for yy in range(YN):
                greet((r - d * ZC, yy))

    @pl.when(jnp.logical_not(first))
    def _():
        for yy in range(YN):
            greet((r - 1, yy))

    @pl.when(jnp.logical_not(last))
    def _():
        for yy in range(YN):
            greet((r + 1, yy))

    row = lax.broadcasted_iota(jnp.int32, (16, NT), 0)
    lane = lax.broadcasted_iota(jnp.int32, (8, NT), 1)
    center = INNER_RADIUS + ((r * RD - 2 + row).astype(jnp.float32) + 0.5) * DR
    square = center * center
    below, above = center - 0.5 * DR, center + 0.5 * DR
    tb[0] = 0.5 * DT * (above * above) / (square * DR)
    tb[1] = 0.5 * DT * (below * below) / (square * DR)
    tb[2] = 1.0 / center
    tb[3] = (STRENGTH * DT) / square
    tb[4] = square

    def at(table, k):
        return tb[table, pl.ds(k + 2, 1), :]

    load.wait()

    weight = polar_ref[4:5, :]
    total = None
    for k in range(RD):
        part = e0[0, 2 + k, PAD : PAD + 8, :] + e0[0, 2 + k, PAD + 8 : PAD + 16, :]
        part = jnp.sum(part, axis=0, keepdims=True) * weight * at(4, k)
        rows_src[k : k + 1, :] = part
        total = part if total is None else total + part
    l1_in[pl.ds(zc, 1)] = total[None]
    rows_in[1, pl.ds(y, 1)] = rows_src[...][None]

    count = ZC - 1 + YN - 1 + YN * (XN - 1 - xi)
    count = count + jnp.where(first, 0, YN) + jnp.where(last, 0, YN)
    pl.semaphore_wait(barrier, count)

    def halo(e, base, which):
        phi_rows, own = pl.ds(2, RD), pl.ds(PAD, NW)
        src, dst, device = (
            (e.at[:, phi_rows, pl.ds(PAD, 2), :], e.at[:, phi_rows, pl.ds(PAD + NW, 2), :], (r, lax.rem(y + YN - 1, YN))),
            (e.at[:, phi_rows, pl.ds(PAD + NW - 2, 2), :], e.at[:, phi_rows, pl.ds(PAD - 2, 2), :], (r, lax.rem(y + 1, YN))),
            (e.at[:, pl.ds(2, 2), own, :], e.at[:, pl.ds(2 + RD, 2), own, :], (r - 1, y)),
            (e.at[:, pl.ds(RD, 2), own, :], e.at[:, pl.ds(0, 2), own, :], (r + 1, y)),
        )[which]
        return pltpu.make_async_remote_copy(
            src_ref=src, dst_ref=dst, send_sem=h_send.at[base + which], recv_sem=h_recv.at[base + which],
            device_id=device, device_id_type=MESH,
        )

    def start_halos(e, base):
        pl.when(jnp.logical_not(first))(lambda: halo(e, base, 2).start())
        pl.when(jnp.logical_not(last))(lambda: halo(e, base, 3).start())
        halo(e, base, 0).start()
        halo(e, base, 1).start()

    def wait_halos(e, base):
        pl.when(jnp.logical_not(last))(lambda: halo(e, base, 2).wait_recv())
        pl.when(jnp.logical_not(first))(lambda: halo(e, base, 3).wait_recv())
        halo(e, base, 0).wait_recv()
        halo(e, base, 1).wait_recv()

    def wait_sent(e, base):
        pl.when(jnp.logical_not(first))(lambda: halo(e, base, 2).wait_send())
        pl.when(jnp.logical_not(last))(lambda: halo(e, base, 3).wait_send())
        halo(e, base, 0).wait_send()
        halo(e, base, 1).wait_send()

    def line_copy(d):
        return pltpu.make_async_remote_copy(
            src_ref=l1_in.at[zc], dst_ref=l1_in.at[zc], send_sem=a_send.at[d], recv_sem=a_recv.at[zc],
            device_id=line[d - 1], device_id_type=MESH,
        )

    def line_arrival(d):
        j = lax.rem(zc + d, ZC)
        return pltpu.make_async_remote_copy(
            src_ref=l1_in.at[j], dst_ref=l1_in.at[j], send_sem=a_send.at[d], recv_sem=a_recv.at[j],
            device_id=line[d - 1], device_id_type=MESH,
        )

    def rows_copy(group, yy, slot, device):
        return pltpu.make_async_remote_copy(
            src_ref=rows_src, dst_ref=rows_in.at[group, slot], send_sem=r_send.at[group * YN + yy],
            recv_sem=r_recv.at[group, slot], device_id=device, device_id_type=MESH,
        )

    for d in range(1, ZC):
        line_copy(d).start()
    start_halos(e0, 0)
    for d in range(1, YN):
        rows_copy(1, d, y, wedge[d - 1]).start()

    @pl.when(jnp.logical_not(first))
    def _():
        for yy in range(YN):
            rows_copy(2, yy, y, (r - 1, yy)).start()

    @pl.when(jnp.logical_not(last))
    def _():
        for yy in range(YN):
            rows_copy(0, yy, y, (r + 1, yy)).start()

    is_first_lane = lane == 0

    def polar_part(e, k, h, gravity):
        rows = pl.ds(PAD + 8 * h, 8)
        u = [e[v, k + 2, rows, :] for v in range(NV)]
        left, right = [], []
        for v in range(NV):
            back = pltpu.roll(u[v], 1, 1)
            diff = jnp.where(is_first_lane, 0.0, u[v] - back)
            slope = 0.5 * minmod(diff, pltpu.roll(diff, NT - 1, 1))
            left.append(pltpu.roll(u[v] + slope, 1, 1))
            right.append(jnp.where(is_first_lane, back, u[v] - slope))
        flux = twice_flux(left, right, 2)
        inverse_r = at(2, k)
        low, high = polar_ref[0:1, :] * inverse_r, polar_ref[1:2, :] * inverse_r
        new = [u[v] - (pltpu.roll(flux[v], NT - 1, 1) * high - flux[v] * low) for v in range(NV)]
        density, inverse, pressure = thermo(u)
        v1, v2, v3 = u[1] * inverse, u[2] * inverse, u[3] * inverse
        cot, step_r = polar_ref[3:4, :], DT * inverse_r
        d3 = density * v3
        d33 = d3 * v3
        new[1] = new[1] + (2.0 * pressure + density * (v2 * v2) + d33) * step_r
        new[2] = new[2] + ((pressure + d33) * cot - density * v1 * v2) * step_r
        new[3] = new[3] - d3 * (v1 + v2 * cot) * step_r
        if gravity:
            pull = gt[pl.ds(k + 2, 1), :]
            new[1] = new[1] - density * pull
            new[4] = new[4] - u[1] * pull
        for v in range(NV):
            acc[v, k, pl.ds(8 * h, 8), :] = new[v]

    def polar_phase(e, gravity):
        def step(k, _):
            for h in range(2):
                polar_part(e, k, h, gravity)
            return 0

        lax.fori_loop(0, RD, step, 0)

    def radial_phase(e):
        def step(h, _):
            rows = pl.ds(pl.multiple_of(PAD + 8 * h, 8), 8)
            mine = pl.ds(pl.multiple_of(8 * h, 8), 8)
            value = [e[v, 1, rows, :] for v in range(NV)]
            diff = [value[v] - e[v, 0, rows, :] for v in range(NV)]
            left = before = None
            for k in range(-1, RD + 1):
                after = [e[v, k + 3, rows, :] for v in range(NV)]
                ahead = [after[v] - value[v] for v in range(NV)]
                slope = [0.5 * minmod(diff[v], ahead[v]) for v in range(NV)]
                if k >= 0:
                    flux = twice_flux(left, [value[v] - slope[v] for v in range(NV)], 1)
                    if k >= 1:
                        up, down = at(0, k - 1), at(1, k - 1)
                        for v in range(NV):
                            acc[v, k - 1, mine, :] = acc[v, k - 1, mine, :] - (flux[v] * up - before[v] * down)
                    before = flux
                left = [value[v] + slope[v] for v in range(NV)]
                value, diff = after, ahead
            return 0

        lax.fori_loop(0, 2, step, 0)

    def azimuth_flux(load_at):
        u = [[load_at(v, s) for v in range(NV)] for s in range(-2, 2)]
        back = [u[1][v] - u[0][v] for v in range(NV)]
        here = [u[2][v] - u[1][v] for v in range(NV)]
        ahead = [u[3][v] - u[2][v] for v in range(NV)]
        left = [u[1][v] + 0.5 * minmod(back[v], here[v]) for v in range(NV)]
        right = [u[2][v] - 0.5 * minmod(here[v], ahead[v]) for v in range(NV)]
        return twice_flux(left, right, 3)

    def azimuth_phase(e, finish):
        flat = e.reshape(NV * 12 * ROWS, NT)
        flux = azimuth_flux(
            lambda v, s: flat[pl.ds((v * 12 + 2) * ROWS + PAD + NW + s, RD, stride=ROWS), :]
        )
        fp_flat = fp.reshape(NV * RD * 24, NT)
        for v in range(NV):
            fp_flat[pl.ds(v * RD * 24 + NW, RD, stride=24), :] = flux[v]

        def step(k, _):
            for h in range(2):
                flux = azimuth_flux(lambda v, s: e[v, k + 2, PAD + 8 * h + s : PAD + 8 * h + s + 8, :])
                for v in range(NV):
                    fp[v, k, 8 * h : 8 * h + 8, :] = flux[v]
            scale = polar_ref[2:3, :] * at(2, k)
            for h in range(2):
                for v in range(NV):
                    net = fp[v, k, 8 * h + 1 : 8 * h + 9, :] - fp[v, k, 8 * h : 8 * h + 8, :]
                    finish(v, k, h, acc[v, k, 8 * h : 8 * h + 8, :] - net * scale)
            return 0

        lax.fori_loop(0, RD, step, 0)

    def edges(e):
        @pl.when(first)
        def _():
            for j in range(2):
                e[:, j, PAD : PAD + NW, :] = e[:, 2, PAD : PAD + NW, :]

        @pl.when(last)
        def _():
            for j in range(2):
                e[:, 2 + RD + j, PAD : PAD + NW, :] = e[:, 1 + RD, PAD : PAD + NW, :]

    polar_phase(e0, False)

    for d in range(1, ZC):
        line_arrival(d).wait_recv()
    whole = inner = None
    for j in range(ZC):
        part = l1_in[j]
        kept = jnp.where(j < zc, part, 0.0)
        whole = part if j == 0 else whole + part
        inner = kept if j == 0 else inner + kept
    l2_src[0:1, :] = whole
    l2_src[1:2, :] = inner
    me = xi * YN + y
    l2_in[pl.ds(me, 1)] = l2_src[...][None]

    def plane_copy(sem, slot, device):
        return pltpu.make_async_remote_copy(
            src_ref=l2_src, dst_ref=l2_in.at[slot], send_sem=b_send.at[sem], recv_sem=b_recv.at[slot],
            device_id=device, device_id_type=MESH,
        )

    for d in range(1, YN):
        plane_copy(d, me, wedge[d - 1]).start()
    for d in range(1, XN):

        @pl.when(xi + d < XN)
        def _(d=d):
            for yy in range(YN):
                plane_copy(d * YN + yy, me, (r + d * ZC, yy)).start()

    wait_halos(e0, 0)
    edges(e0)
    radial_phase(e0)

    def finish_one(v, k, h, value):
        e1[v, k + 2, PAD + 8 * h : PAD + 8 * h + 8, :] = value

    azimuth_phase(e0, finish_one)
    start_halos(e1, 4)

    for d in range(1, YN):
        j = lax.rem(y + d, YN)
        rows_copy(1, d, j, wedge[d - 1]).wait_recv()
        plane_copy(d, xi * YN + j, wedge[d - 1]).wait_recv()

    @pl.when(jnp.logical_not(first))
    def _():
        for yy in range(YN):
            rows_copy(0, yy, yy, (r - 1, yy)).wait_recv()

    @pl.when(jnp.logical_not(last))
    def _():
        for yy in range(YN):
            rows_copy(2, yy, yy, (r + 1, yy)).wait_recv()

    @pl.when(first)
    def _():
        rows_in[0] = jnp.zeros((YN, RD, NT), jnp.float32)

    @pl.when(last)
    def _():
        rows_in[2] = jnp.zeros((YN, RD, NT), jnp.float32)

    for d in range(1, XN):

        @pl.when(xi - d >= 0)
        def _(d=d):
            for yy in range(YN):
                plane_copy(0, (xi - d) * YN + yy, (r - d * ZC, yy)).wait_recv()

    base = None
    for xx in range(XN):
        for yy in range(YN):
            pair = l2_in[xx * YN + yy]
            kept = jnp.where(xx < xi, pair[0:1, :], jnp.where(xx == xi, pair[1:2, :], 0.0))
            base = kept if base is None else base + kept
    inside, own, outside = (rows_in[g, 0] + rows_in[g, 1] + rows_in[g, 2] + rows_in[g, 3] for g in range(3))
    one = [own[k : k + 1, :] for k in range(RD)]
    gt[1:2, :] = base - 0.5 * inside[7:8, :]
    gt[0:1, :] = base - inside[7:8, :] - 0.5 * inside[6:7, :]
    sofar = base
    for k in range(RD):
        gt[k + 2 : k + 3, :] = sofar + 0.5 * one[k]
        sofar = sofar + one[k]
    gt[RD + 2 : RD + 3, :] = sofar + 0.5 * outside[0:1, :]
    gt[RD + 3 : RD + 4, :] = sofar + outside[0:1, :] + 0.5 * outside[1:2, :]
    gt[RD + 4 : 16, :] = jnp.zeros((4, NT), jnp.float32)
    enclosed = jnp.broadcast_to(jnp.sum(gt[...], axis=1, keepdims=True), (16, NT)) + core_ref[0]
    diagonal = lax.broadcasted_iota(jnp.int32, (16, NT), 1) + 2 == row
    enc_v[...] = jnp.sum(jnp.where(diagonal, enclosed, 0.0), axis=0, keepdims=True)
    gt[...] = enclosed * tb[3]
    enc_out = pltpu.make_async_copy(enc_v.at[:, pl.ds(0, NT)], enc_ref, enc_sem)
    enc_out.start()

    def pull_down(k, rows):
        pull = gt[pl.ds(k + 2, 1), :]
        density = jnp.maximum(e0[0, k + 2, rows, :], MINIMUM_DENSITY)
        e1[1, k + 2, rows, :] = e1[1, k + 2, rows, :] - density * pull
        e1[4, k + 2, rows, :] = e1[4, k + 2, rows, :] - e0[1, k + 2, rows, :] * pull

    wait_sent(e1, 4)
    for k in range(RD):
        pull_down(k, pl.ds(PAD, NW))

    polar_phase(e1, True)
    wait_halos(e1, 4)
    for k in range(RD):
        pull_down(k, pl.ds(PAD - 2, 2))
        pull_down(k, pl.ds(PAD + NW, 2))
    for k in (-2, -1, RD, RD + 1):
        pull_down(k, pl.ds(PAD, NW))
    edges(e1)
    radial_phase(e1)

    def finish_two(v, k, h, value):
        out_v[v, k, 8 * h : 8 * h + 8, :] = 0.5 * (e0[v, k + 2, PAD + 8 * h : PAD + 8 * h + 8, :] + value)

    azimuth_phase(e1, finish_two)
    store = pltpu.make_async_copy(out_v, out_ref, out_sem)
    store.start()

    wait_sent(e0, 0)
    for d in range(1, ZC):
        line_copy(d).wait_send()
    for d in range(1, YN):
        rows_copy(1, d, y, wedge[d - 1]).wait_send()
        plane_copy(d, me, wedge[d - 1]).wait_send()

    @pl.when(jnp.logical_not(first))
    def _():
        for yy in range(YN):
            rows_copy(2, yy, y, (r - 1, yy)).wait_send()

    @pl.when(jnp.logical_not(last))
    def _():
        for yy in range(YN):
            rows_copy(0, yy, y, (r + 1, yy)).wait_send()

    for d in range(1, XN):

        @pl.when(xi + d < XN)
        def _(d=d):
            for yy in range(YN):
                plane_copy(d * YN + yy, me, (r + d * ZC, yy)).wait_send()

    enc_out.wait()
    store.wait()


def body(conserved, core_mass):
    f32 = jnp.float32
    dma = pltpu.SemaphoreType.DMA
    vmem = pltpu.VMEM
    extended = vmem((NV, RD + 4, ROWS, NT), f32)
    slab = vmem((NV, RD, NW, NT), f32)
    advanced, enclosed = pl.pallas_call(
        kernel,
        out_shape=(
            jax.ShapeDtypeStruct(conserved.shape, f32),
            jax.ShapeDtypeStruct((1, NT), f32),
        ),
        in_specs=[
            pl.BlockSpec(memory_space=pl.ANY),
            pl.BlockSpec(memory_space=pltpu.SMEM),
            pl.BlockSpec(memory_space=vmem),
        ],
        out_specs=(pl.BlockSpec(memory_space=pl.ANY), pl.BlockSpec(memory_space=pl.ANY)),
        scratch_shapes=[
            extended, extended, slab, vmem((NV, RD, 24, NT), f32), slab,
            vmem((5, 16, NT), f32), vmem((16, NT), f32), vmem((1, NT), f32),
            vmem((RD, NT), f32), vmem((3, YN, RD, NT), f32),
            vmem((ZC, 1, NT), f32), vmem((2, NT), f32), vmem((XN * YN, 2, NT), f32),
            dma, dma, dma, dma((8,)), dma((8,)), dma((3 * YN,)), dma((3, YN)),
            dma((ZC,)), dma((ZC,)), dma((XN * YN,)), dma((XN * YN,)),
        ],
        compiler_params=pltpu.CompilerParams(collective_id=0, has_side_effects=True),
        name="step",
    )(conserved, core_mass, jnp.asarray(polar_table()))
    return advanced, enclosed[0, :RD]


def solution(mesh):
    in_specs = (P(None, "radial", "phi", None), P())
    out_specs = (P(None, "radial", "phi", None), P("radial"))
    return jax.shard_map(body, mesh=mesh, in_specs=in_specs, out_specs=out_specs, check_vma=False)
```

```python
import math

import jax
import jax.numpy as jnp
import numpy as np
from jax import lax
from jax.experimental import pallas as pl
from jax.experimental.pallas import tpu as pltpu
from jax.sharding import PartitionSpec as P

ADIABATIC = 4.0 / 3.0
INNER_RADIUS = 1.0
OUTER_RADIUS = 2.0
COURANT = 0.4
GRAVITY_KICK = 0.004
MINIMUM_DENSITY = 0.05
PRESSURE_FLOOR = 0.01

MESH = pl.DeviceIdType.MESH
NV = 8
RD = 8
NW = 16
NT = 128
PAD = 8
ROWS = 32
XN, ZC, YN = 4, 16, 4
RADIAL = XN * ZC
VMEM_LIMIT = 24 << 20


def step_sizes(radial_total, phi_total, theta_total):
    theta_step = math.pi / theta_total
    phi_step = 2.0 * math.pi / phi_total
    polar_width = INNER_RADIUS * math.sin(0.5 * theta_step) * phi_step
    radial_step = min(2.0 * polar_width, (OUTER_RADIUS - INNER_RADIUS) / radial_total)
    timestep = COURANT * min(radial_step, polar_width)
    return (radial_step, theta_step, phi_step, timestep)


DR, DTH, DPH, DT = step_sizes(RADIAL * RD, YN * NW, NT)
STRENGTH = GRAVITY_KICK / DT


def polar_table():
    center = (np.arange(NT) + 0.5) * DTH
    face = np.arange(NT + 1) * DTH
    sine, face_sine = np.sin(center), np.sin(face)
    table = np.zeros((8, NT))
    table[0] = 0.5 * DT * face_sine[:-1] / (sine * DTH)
    table[1] = 0.5 * DT * face_sine[1:] / (sine * DTH)
    table[2] = 0.5 * DT / (sine * DPH)
    table[3] = np.cos(center) / sine
    table[4] = sine * (DR * DTH * DPH)
    return table.astype(np.float32)


def thermo(u):
    density = jnp.maximum(u[0], MINIMUM_DENSITY)
    inverse = 1.0 / density
    kinetic = 0.5 * (u[1] * u[1] + u[2] * u[2] + u[3] * u[3]) * inverse
    pressure = jnp.maximum((ADIABATIC - 1.0) * (u[4] - kinetic), PRESSURE_FLOOR * density)
    return density, inverse, pressure


def side(u, m):
    _, inverse, pressure = thermo(u)
    normal = u[m] * inverse
    square = ADIABATIC * pressure * inverse
    return pressure, normal, jnp.abs(normal) + square * lax.rsqrt(square)


def minmod(a, b):
    return jnp.maximum(jnp.minimum(a, b), jnp.minimum(jnp.maximum(a, b), 0.0))


def twice_flux(left, right, m):
    pl_, vl, al = side(left, m)
    pr_, vr, ar = side(right, m)
    signal = jnp.maximum(al, ar)
    cl, cr = vl + signal, vr - signal
    flux = [cl * a + cr * b for a, b in zip(left, right)]
    flux[m] = flux[m] + (pl_ + pr_)
    flux[4] = flux[4] + (pl_ * vl + pr_ * vr)
    return flux


def at(tb, table, k):
    return tb[table, pl.ds(k + 2, 1), :]


def polar_phase(e, acc, tb, polar, gt):
    is_first_lane = lax.broadcasted_iota(jnp.int32, (8, NT), 1) == 0

    def tile(k, h):
        u = [e[v, k + 2, PAD + 8 * h : PAD + 8 * h + 8, :] for v in range(NV)]
        left, right = [], []
        for v in range(NV):
            back = pltpu.roll(u[v], 1, 1)
            diff = jnp.where(is_first_lane, 0.0, u[v] - back)
            slope = 0.5 * minmod(diff, pltpu.roll(diff, NT - 1, 1))
            left.append(pltpu.roll(u[v] + slope, 1, 1))
            right.append(jnp.where(is_first_lane, back, u[v] - slope))
        flux = twice_flux(left, right, 2)
        inverse_r = at(tb, 2, k)
        low, high = polar[0:1, :] * inverse_r, polar[1:2, :] * inverse_r
        new = [u[v] - (pltpu.roll(flux[v], NT - 1, 1) * high - flux[v] * low) for v in range(NV)]
        density, inverse, pressure = thermo(u)
        v1, v2, v3 = u[1] * inverse, u[2] * inverse, u[3] * inverse
        cot, step_r = polar[3:4, :], DT * inverse_r
        d3 = density * v3
        d33 = d3 * v3
        new[1] = new[1] + (2.0 * pressure + density * (v2 * v2) + d33) * step_r
        new[2] = new[2] + ((pressure + d33) * cot - density * v1 * v2) * step_r
        new[3] = new[3] - d3 * (v1 + v2 * cot) * step_r
        if gt is not None:
            pull = gt[pl.ds(k + 2, 1), :]
            new[1] = new[1] - density * pull
            new[4] = new[4] - u[1] * pull
        for v in range(NV):
            acc[v, k, 8 * h : 8 * h + 8, :] = new[v]

    def step(k, _):
        for h in range(2):
            tile(k, h)
        return 0

    lax.fori_loop(0, RD, step, 0)


def radial_faces(e, rf, spans):
    def step(h, _):
        rows = pl.ds(pl.multiple_of(PAD + 8 * h, 8), 8)
        mine = pl.ds(pl.multiple_of(8 * h, 8), 8)
        for begin, end in spans:
            value = [e[v, begin + 1, rows, :] for v in range(NV)]
            diff = [value[v] - e[v, begin, rows, :] for v in range(NV)]
            left = None
            for k in range(begin - 1, end):
                after = [e[v, k + 3, rows, :] for v in range(NV)]
                ahead = [after[v] - value[v] for v in range(NV)]
                slope = [0.5 * minmod(diff[v], ahead[v]) for v in range(NV)]
                if k >= begin:
                    flux = twice_flux(left, [value[v] - slope[v] for v in range(NV)], 1)
                    for v in range(NV):
                        rf[v, k, mine, :] = flux[v]
                left = [value[v] + slope[v] for v in range(NV)]
                value, diff = after, ahead
        return 0

    lax.fori_loop(0, 2, step, 0)


def azimuth_flux(load_at):
    u = [[load_at(v, s) for v in range(NV)] for s in range(-2, 2)]
    back = [u[1][v] - u[0][v] for v in range(NV)]
    here = [u[2][v] - u[1][v] for v in range(NV)]
    ahead = [u[3][v] - u[2][v] for v in range(NV)]
    left = [u[1][v] + 0.5 * minmod(back[v], here[v]) for v in range(NV)]
    right = [u[2][v] - 0.5 * minmod(here[v], ahead[v]) for v in range(NV)]
    return twice_flux(left, right, 3)


def azimuth_inner(e, fp):
    def step(k, _):
        for face in (2, 7):
            flux = azimuth_flux(lambda v, s: e[v, k + 2, PAD + face + s : PAD + face + s + 8, :])
            for v in range(NV):
                fp[v, k, face : face + 8, :] = flux[v]
        return 0

    lax.fori_loop(0, RD, step, 0)


def azimuth_outer(e, fp):
    flat = e.reshape(NV * 12 * ROWS, NT)
    fp_flat = fp.reshape(NV * RD * 24, NT)
    for face in (0, 1, NW - 1, NW):
        flux = azimuth_flux(
            lambda v, s: flat[pl.ds((v * 12 + 2) * ROWS + PAD + face + s, RD, stride=ROWS), :]
        )
        for v in range(NV):
            fp_flat[pl.ds(v * RD * 24 + face, RD, stride=24), :] = flux[v]


def finish_zones(acc, rf, fp, tb, polar, put, row_done):
    for k in range(RD):
        up, down = at(tb, 0, k), at(tb, 1, k)
        scale = polar[2:3, :] * at(tb, 2, k)
        for h in range(2):
            mine = slice(8 * h, 8 * h + 8)
            for v in range(NV):
                radial = rf[v, k + 1, mine, :] * up - rf[v, k, mine, :] * down
                azimuth = (fp[v, k, 8 * h + 1 : 8 * h + 9, :] - fp[v, k, mine, :]) * scale
                put(v, k, h, acc[v, k, mine, :] - radial - azimuth)
        if row_done is not None:
            row_done(k)


def kernel(
    x_ref, core_ref, polar_hbm, e0, acc, rf, fp, tb, polar, enc_v,
    e1, gt, rows_src, rows_in, l1_in, l2_src, l2_in,
    load_sem, h_send, h_recv, r_send, r_recv, a_send, a_recv, b_send, b_recv,
):
    r, y = lax.axis_index("radial"), lax.axis_index("phi")
    zc, xi = lax.rem(r, ZC), r // ZC
    first, last = r == 0, r == RADIAL - 1
    inner_there, outer_there = jnp.logical_not(first), jnp.logical_not(last)

    load = pltpu.make_async_copy(x_ref, e0.at[:, 2 : 2 + RD, PAD : PAD + NW, :], load_sem.at[0])
    polar_load = pltpu.make_async_copy(polar_hbm, polar, load_sem.at[1])
    load.start()
    polar_load.start()

    line = [(xi * ZC + lax.rem(zc + d, ZC), y) for d in range(1, ZC)]
    wedge = [(r, lax.rem(y + d, YN)) for d in range(1, YN)]
    barrier = pltpu.get_barrier_semaphore()

    def greet(device):
        pl.semaphore_signal(barrier, inc=1, device_id=device, device_id_type=MESH)

    for device in line + wedge:
        greet(device)

    def greet_all(slab):
        for yy in range(YN):
            greet((slab, yy))

    for d in range(1, XN):
        pl.when(xi - d >= 0)(lambda d=d: greet_all(r - d * ZC))
    pl.when(inner_there)(lambda: greet_all(r - 1))
    pl.when(outer_there)(lambda: greet_all(r + 1))

    row = lax.broadcasted_iota(jnp.int32, (16, NT), 0)
    center = INNER_RADIUS + ((r * RD - 2 + row).astype(jnp.float32) + 0.5) * DR
    square = center * center
    below, above = center - 0.5 * DR, center + 0.5 * DR
    tb[0] = 0.5 * DT * (above * above) / (square * DR)
    tb[1] = 0.5 * DT * (below * below) / (square * DR)
    tb[2] = 1.0 / center
    tb[3] = (STRENGTH * DT) / square
    tb[4] = square

    polar_load.wait()
    load.wait()

    weight = polar[4:5, :]
    total = None
    for k in range(RD):
        part = e0[0, 2 + k, PAD : PAD + 8, :] + e0[0, 2 + k, PAD + 8 : PAD + 16, :]
        part = jnp.sum(part, axis=0, keepdims=True) * weight * at(tb, 4, k)
        rows_src[k : k + 1, :] = part
        total = part if total is None else total + part
    l1_in[pl.ds(zc, 1)] = total[None]
    rows_in[1, pl.ds(y, 1)] = rows_src[...][None]

    count = ZC - 1 + YN - 1 + YN * (XN - 1 - xi)
    count = count + jnp.where(first, 0, YN) + jnp.where(last, 0, YN)
    pl.semaphore_wait(barrier, count)

    def remote(src, dst, send, recv, device):
        return pltpu.make_async_remote_copy(
            src_ref=src, dst_ref=dst, send_sem=send, recv_sem=recv, device_id=device, device_id_type=MESH
        )

    def halo(e, base, which):
        phi_rows, own = pl.ds(2, RD), pl.ds(PAD, NW)
        src, dst, device = (
            (e.at[:, phi_rows, pl.ds(PAD, 2), :], e.at[:, phi_rows, pl.ds(PAD + NW, 2), :], (r, lax.rem(y + YN - 1, YN))),
            (e.at[:, phi_rows, pl.ds(PAD + NW - 2, 2), :], e.at[:, phi_rows, pl.ds(PAD - 2, 2), :], (r, lax.rem(y + 1, YN))),
            (e.at[:, pl.ds(2, 2), own, :], e.at[:, pl.ds(2 + RD, 2), own, :], (r - 1, y)),
            (e.at[:, pl.ds(RD, 2), own, :], e.at[:, pl.ds(0, 2), own, :], (r + 1, y)),
        )[which]
        return remote(src, dst, h_send.at[base + which], h_recv.at[base + which], device)

    def start_halos(e, base):
        pl.when(inner_there)(lambda: halo(e, base, 2).start())
        pl.when(outer_there)(lambda: halo(e, base, 3).start())
        halo(e, base, 0).start()
        halo(e, base, 1).start()

    def wait_halos(e, base):
        pl.when(outer_there)(lambda: halo(e, base, 2).wait_recv())
        pl.when(inner_there)(lambda: halo(e, base, 3).wait_recv())
        halo(e, base, 0).wait_recv()
        halo(e, base, 1).wait_recv()

    def wait_sent(e, base):
        pl.when(inner_there)(lambda: halo(e, base, 2).wait_send())
        pl.when(outer_there)(lambda: halo(e, base, 3).wait_send())
        halo(e, base, 0).wait_send()
        halo(e, base, 1).wait_send()

    def line_copy(d):
        return remote(l1_in.at[zc], l1_in.at[zc], a_send.at[d], a_recv.at[zc], line[d - 1])

    def line_arrival(d):
        j = lax.rem(zc + d, ZC)
        return remote(l1_in.at[j], l1_in.at[j], a_send.at[d], a_recv.at[j], line[d - 1])

    def rows_copy(group, sem, slot, device):
        return remote(rows_src, rows_in.at[group, slot], r_send.at[group * YN + sem], r_recv.at[group, slot], device)

    for d in range(1, ZC):
        line_copy(d).start()
    start_halos(e0, 0)
    for d in range(1, YN):
        rows_copy(1, d, y, wedge[d - 1]).start()

    def each_wedge(act):
        for yy in range(YN):
            act(yy)

    pl.when(inner_there)(lambda: each_wedge(lambda yy: rows_copy(2, yy, y, (r - 1, yy)).start()))
    pl.when(outer_there)(lambda: each_wedge(lambda yy: rows_copy(0, yy, y, (r + 1, yy)).start()))

    def edges(e):
        @pl.when(first)
        def _():
            for j in range(2):
                e[:, j, PAD : PAD + NW, :] = e[:, 2, PAD : PAD + NW, :]

        @pl.when(last)
        def _():
            for j in range(2):
                e[:, 2 + RD + j, PAD : PAD + NW, :] = e[:, 1 + RD, PAD : PAD + NW, :]

    polar_phase(e0, acc, tb, polar, None)
    radial_faces(e0, rf, ((2, RD - 1),))
    azimuth_inner(e0, fp)

    for d in range(1, ZC):
        line_arrival(d).wait_recv()
    whole = inner = None
    for j in range(ZC):
        part = l1_in[j]
        kept = jnp.where(j < zc, part, 0.0)
        whole = part if j == 0 else whole + part
        inner = kept if j == 0 else inner + kept
    l2_src[0:1, :] = whole
    l2_src[1:2, :] = inner
    me = xi * YN + y
    l2_in[pl.ds(me, 1)] = l2_src[...][None]

    def plane_copy(sem, slot, device):
        return remote(l2_src, l2_in.at[slot], b_send.at[sem], b_recv.at[slot], device)

    for d in range(1, YN):
        plane_copy(d, me, wedge[d - 1]).start()
    for d in range(1, XN):
        pl.when(xi + d < XN)(
            lambda d=d: each_wedge(lambda yy: plane_copy(d * YN + yy, me, (r + d * ZC, yy)).start())
        )

    wait_halos(e0, 0)
    edges(e0)
    radial_faces(e0, rf, ((0, 2), (RD - 1, RD + 1)))
    azimuth_outer(e0, fp)

    def put(v, k, h, value):
        e1[v, k + 2, PAD + 8 * h : PAD + 8 * h + 8, :] = value

    finish_zones(acc, rf, fp, tb, polar, put, None)
    start_halos(e1, 4)

    for d in range(1, YN):
        j = lax.rem(y + d, YN)
        rows_copy(1, d, j, wedge[d - 1]).wait_recv()
        plane_copy(d, xi * YN + j, wedge[d - 1]).wait_recv()
    pl.when(inner_there)(lambda: each_wedge(lambda yy: rows_copy(0, yy, yy, (r - 1, yy)).wait_recv()))
    pl.when(outer_there)(lambda: each_wedge(lambda yy: rows_copy(2, yy, yy, (r + 1, yy)).wait_recv()))

    @pl.when(first)
    def _():
        rows_in[0] = jnp.zeros((YN, RD, NT), jnp.float32)

    @pl.when(last)
    def _():
        rows_in[2] = jnp.zeros((YN, RD, NT), jnp.float32)

    for d in range(1, XN):
        pl.when(xi - d >= 0)(
            lambda d=d: each_wedge(
                lambda yy: plane_copy(0, (xi - d) * YN + yy, (r - d * ZC, yy)).wait_recv()
            )
        )

    base = None
    for xx in range(XN):
        for yy in range(YN):
            pair = l2_in[xx * YN + yy]
            kept = jnp.where(xx < xi, pair[0:1, :], jnp.where(xx == xi, pair[1:2, :], 0.0))
            base = kept if base is None else base + kept
    inside, own, outside = (rows_in[g, 0] + rows_in[g, 1] + rows_in[g, 2] + rows_in[g, 3] for g in range(3))
    one = [own[k : k + 1, :] for k in range(RD)]
    gt[1:2, :] = base - 0.5 * inside[7:8, :]
    gt[0:1, :] = base - inside[7:8, :] - 0.5 * inside[6:7, :]
    sofar = base
    for k in range(RD):
        gt[k + 2 : k + 3, :] = sofar + 0.5 * one[k]
        sofar = sofar + one[k]
    gt[RD + 2 : RD + 3, :] = sofar + 0.5 * outside[0:1, :]
    gt[RD + 3 : RD + 4, :] = sofar + outside[0:1, :] + 0.5 * outside[1:2, :]
    gt[RD + 4 : 16, :] = jnp.zeros((4, NT), jnp.float32)
    enclosed = jnp.broadcast_to(jnp.sum(gt[...], axis=1, keepdims=True), (16, NT)) + core_ref[0]
    diagonal = lax.broadcasted_iota(jnp.int32, (16, NT), 1) + 2 == row
    enc_v[...] = jnp.sum(jnp.where(diagonal, enclosed, 0.0), axis=0, keepdims=True)
    gt[...] = enclosed * tb[3]

    def pull_down(k, rows):
        pull = gt[pl.ds(k + 2, 1), :]
        density = jnp.maximum(e0[0, k + 2, rows, :], MINIMUM_DENSITY)
        e1[1, k + 2, rows, :] = e1[1, k + 2, rows, :] - density * pull
        e1[4, k + 2, rows, :] = e1[4, k + 2, rows, :] - e0[1, k + 2, rows, :] * pull

    wait_sent(e1, 4)
    for k in range(RD):
        pull_down(k, pl.ds(PAD, NW))

    polar_phase(e1, acc, tb, polar, gt)
    radial_faces(e1, rf, ((2, RD - 1),))
    azimuth_inner(e1, fp)
    wait_halos(e1, 4)
    for k in range(RD):
        pull_down(k, pl.ds(PAD - 2, 2))
        pull_down(k, pl.ds(PAD + NW, 2))
    for k in (-2, -1, RD, RD + 1):
        pull_down(k, pl.ds(PAD, NW))
    edges(e1)
    radial_faces(e1, rf, ((0, 2), (RD - 1, RD + 1)))
    azimuth_outer(e1, fp)

    wait_sent(e0, 0)
    for d in range(1, ZC):
        line_copy(d).wait_send()
    for d in range(1, YN):
        rows_copy(1, d, y, wedge[d - 1]).wait_send()
        plane_copy(d, me, wedge[d - 1]).wait_send()
    pl.when(inner_there)(lambda: each_wedge(lambda yy: rows_copy(2, yy, y, (r - 1, yy)).wait_send()))
    pl.when(outer_there)(lambda: each_wedge(lambda yy: rows_copy(0, yy, y, (r + 1, yy)).wait_send()))
    for d in range(1, XN):
        pl.when(xi + d < XN)(
            lambda d=d: each_wedge(lambda yy: plane_copy(d * YN + yy, me, (r + d * ZC, yy)).wait_send())
        )


def last_kernel(e0, acc, rf, fp, tb, polar, enc_v, out_ref, enc_ref, out_v, sem):
    enc_ref[...] = enc_v[0, :][:RD]

    def put(v, k, h, value):
        out_v[v, k, 8 * h : 8 * h + 8, :] = 0.5 * (e0[v, k + 2, PAD + 8 * h : PAD + 8 * h + 8, :] + value)

    def store(k):
        return pltpu.make_async_copy(out_v.at[:, k], out_ref.at[:, k], sem.at[k])

    finish_zones(acc, rf, fp, tb, polar, put, lambda k: store(k).start())
    for k in range(RD):
        store(k).wait()


def body(conserved, core_mass):
    f32 = jnp.float32
    dma = pltpu.SemaphoreType.DMA
    vmem, anywhere = pltpu.VMEM, pl.BlockSpec(memory_space=pl.ANY)
    resident = pl.BlockSpec(memory_space=vmem)
    polar = pltpu.with_memory_space_constraint(jnp.asarray(polar_table()), pltpu.HBM)
    conserved = pltpu.with_memory_space_constraint(conserved, pltpu.HBM)
    extended = vmem((NV, RD + 4, ROWS, NT), f32)
    slab = vmem((NV, RD, NW, NT), f32)
    radial_flux, azimuth_fluxes = vmem((NV, RD + 1, NW, NT), f32), vmem((NV, RD, 24, NT), f32)
    held = pl.pallas_call(
        kernel,
        out_shape=(
            extended, slab, radial_flux, azimuth_fluxes, vmem((5, 16, NT), f32), vmem((8, NT), f32), vmem((1, NT), f32),
        ),
        in_specs=[anywhere, pl.BlockSpec(memory_space=pltpu.SMEM), anywhere],
        out_specs=(resident,) * 7,
        scratch_shapes=[
            extended, vmem((16, NT), f32),
            vmem((RD, NT), f32), vmem((3, YN, RD, NT), f32),
            vmem((ZC, 1, NT), f32), vmem((2, NT), f32), vmem((XN * YN, 2, NT), f32),
            dma((2,)), dma((8,)), dma((8,)), dma((3 * YN,)), dma((3, YN)),
            dma((ZC,)), dma((ZC,)), dma((XN * YN,)), dma((XN * YN,)),
        ],
        compiler_params=pltpu.CompilerParams(
            collective_id=0, has_side_effects=True, vmem_limit_bytes=VMEM_LIMIT
        ),
        name="two_sections",
    )(conserved, core_mass, polar)
    e0, acc, rf, fp, tb, polar, enc_v = (pltpu.with_memory_space_constraint(a, vmem) for a in held)
    return pl.pallas_call(
        last_kernel,
        out_shape=(jax.ShapeDtypeStruct(conserved.shape, f32), jax.ShapeDtypeStruct((RD,), f32)),
        in_specs=[resident] * 7,
        out_specs=(anywhere, resident),
        scratch_shapes=[slab, dma((RD,))],
        compiler_params=pltpu.CompilerParams(vmem_limit_bytes=VMEM_LIMIT),
        name="last_faces",
    )(e0, acc, rf, fp, tb, polar, enc_v)


def solution(mesh):
    in_specs = (P(None, "radial", "phi", None), P())
    out_specs = (P(None, "radial", "phi", None), P("radial"))
    return jax.shard_map(body, mesh=mesh, in_specs=in_specs, out_specs=out_specs, check_vma=False)
```

```python
import math

import jax
import jax.numpy as jnp
import numpy as np
from jax import lax
from jax.experimental import pallas as pl
from jax.experimental.pallas import tpu as pltpu
from jax.sharding import PartitionSpec as P

ADIABATIC = 4.0 / 3.0
INNER_RADIUS = 1.0
OUTER_RADIUS = 2.0
COURANT = 0.4
GRAVITY_KICK = 0.004
MINIMUM_DENSITY = 0.05
PRESSURE_FLOOR = 0.01

MESH = pl.DeviceIdType.MESH
NV = 8
RD = 8
NW = 16
NT = 128
PAD = 8
ROWS = 32
XN, ZC, YN = 4, 16, 4
RADIAL = XN * ZC
VMEM_LIMIT = 24 << 20


def step_sizes(radial_total, phi_total, theta_total):
    theta_step = math.pi / theta_total
    phi_step = 2.0 * math.pi / phi_total
    polar_width = INNER_RADIUS * math.sin(0.5 * theta_step) * phi_step
    radial_step = min(2.0 * polar_width, (OUTER_RADIUS - INNER_RADIUS) / radial_total)
    timestep = COURANT * min(radial_step, polar_width)
    return (radial_step, theta_step, phi_step, timestep)


DR, DTH, DPH, DT = step_sizes(RADIAL * RD, YN * NW, NT)
STRENGTH = GRAVITY_KICK / DT


def polar_table():
    center = (np.arange(NT) + 0.5) * DTH
    face = np.arange(NT + 1) * DTH
    sine, face_sine = np.sin(center), np.sin(face)
    table = np.zeros((8, NT))
    table[0] = 0.5 * DT * face_sine[:-1] / (sine * DTH)
    table[1] = 0.5 * DT * face_sine[1:] / (sine * DTH)
    table[2] = 0.5 * DT / (sine * DPH)
    table[3] = np.cos(center) / sine
    table[4] = sine * (DR * DTH * DPH)
    return table.astype(np.float32)


def thermo(u):
    density = jnp.maximum(u[0], MINIMUM_DENSITY)
    inverse = 1.0 / density
    kinetic = 0.5 * (u[1] * u[1] + u[2] * u[2] + u[3] * u[3]) * inverse
    pressure = jnp.maximum((ADIABATIC - 1.0) * (u[4] - kinetic), PRESSURE_FLOOR * density)
    return density, inverse, pressure


def side(u, m):
    _, inverse, pressure = thermo(u)
    normal = u[m] * inverse
    square = ADIABATIC * pressure * inverse
    return pressure, normal, jnp.abs(normal) + square * lax.rsqrt(square)


def minmod(a, b):
    return jnp.maximum(jnp.minimum(a, b), jnp.minimum(jnp.maximum(a, b), 0.0))


def twice_flux(left, right, m):
    pl_, vl, al = side(left, m)
    pr_, vr, ar = side(right, m)
    signal = jnp.maximum(al, ar)
    cl, cr = vl + signal, vr - signal
    flux = [cl * a + cr * b for a, b in zip(left, right)]
    flux[m] = flux[m] + (pl_ + pr_)
    flux[4] = flux[4] + (pl_ * vl + pr_ * vr)
    return flux


def at(tb, table, k):
    return tb[table, pl.ds(k + 2, 1), :]


def polar_phase(e, acc, tb, polar, gt):
    is_first_lane = lax.broadcasted_iota(jnp.int32, (8, NT), 1) == 0

    def tile(k, h):
        u = [e[v, k + 2, PAD + 8 * h : PAD + 8 * h + 8, :] for v in range(NV)]
        left, right = [], []
        for v in range(NV):
            back = pltpu.roll(u[v], 1, 1)
            diff = jnp.where(is_first_lane, 0.0, u[v] - back)
            slope = 0.5 * minmod(diff, pltpu.roll(diff, NT - 1, 1))
            left.append(pltpu.roll(u[v] + slope, 1, 1))
            right.append(jnp.where(is_first_lane, back, u[v] - slope))
        flux = twice_flux(left, right, 2)
        inverse_r = at(tb, 2, k)
        low, high = polar[0:1, :] * inverse_r, polar[1:2, :] * inverse_r
        new = [u[v] - (pltpu.roll(flux[v], NT - 1, 1) * high - flux[v] * low) for v in range(NV)]
        density, inverse, pressure = thermo(u)
        v1, v2, v3 = u[1] * inverse, u[2] * inverse, u[3] * inverse
        cot, step_r = polar[3:4, :], DT * inverse_r
        d3 = density * v3
        d33 = d3 * v3
        new[1] = new[1] + (2.0 * pressure + density * (v2 * v2) + d33) * step_r
        new[2] = new[2] + ((pressure + d33) * cot - density * v1 * v2) * step_r
        new[3] = new[3] - d3 * (v1 + v2 * cot) * step_r
        if gt is not None:
            pull = gt[pl.ds(k + 2, 1), :]
            new[1] = new[1] - density * pull
            new[4] = new[4] - u[1] * pull
        for v in range(NV):
            acc[v, k, 8 * h : 8 * h + 8, :] = new[v]

    def step(k, _):
        for h in range(2):
            tile(k, h)
        return 0

    lax.fori_loop(0, RD, step, 0, unroll=4)


def radial_faces(e, rf, spans):
    def step(h, _):
        rows = pl.ds(pl.multiple_of(PAD + 8 * h, 8), 8)
        mine = pl.ds(pl.multiple_of(8 * h, 8), 8)
        for begin, end in spans:
            value = [e[v, begin + 1, rows, :] for v in range(NV)]
            diff = [value[v] - e[v, begin, rows, :] for v in range(NV)]
            left = None
            for k in range(begin - 1, end):
                after = [e[v, k + 3, rows, :] for v in range(NV)]
                ahead = [after[v] - value[v] for v in range(NV)]
                slope = [0.5 * minmod(diff[v], ahead[v]) for v in range(NV)]
                if k >= begin:
                    flux = twice_flux(left, [value[v] - slope[v] for v in range(NV)], 1)
                    for v in range(NV):
                        rf[v, k, mine, :] = flux[v]
                left = [value[v] + slope[v] for v in range(NV)]
                value, diff = after, ahead
        return 0

    lax.fori_loop(0, 2, step, 0)


def azimuth_flux(load_at):
    u = [[load_at(v, s) for v in range(NV)] for s in range(-2, 2)]
    back = [u[1][v] - u[0][v] for v in range(NV)]
    here = [u[2][v] - u[1][v] for v in range(NV)]
    ahead = [u[3][v] - u[2][v] for v in range(NV)]
    left = [u[1][v] + 0.5 * minmod(back[v], here[v]) for v in range(NV)]
    right = [u[2][v] - 0.5 * minmod(here[v], ahead[v]) for v in range(NV)]
    return twice_flux(left, right, 3)


def azimuth_inner(e, fp):
    def step(k, _):
        for face in (2, 7):
            flux = azimuth_flux(lambda v, s: e[v, k + 2, PAD + face + s : PAD + face + s + 8, :])
            for v in range(NV):
                fp[v, k, face : face + 8, :] = flux[v]
        return 0

    lax.fori_loop(0, RD, step, 0)


def azimuth_outer(e, fp):
    flat = e.reshape(NV * 12 * ROWS, NT)
    fp_flat = fp.reshape(NV * RD * 24, NT)
    for face in (0, 1, NW - 1, NW):
        flux = azimuth_flux(
            lambda v, s: flat[pl.ds((v * 12 + 2) * ROWS + PAD + face + s, RD, stride=ROWS), :]
        )
        for v in range(NV):
            fp_flat[pl.ds(v * RD * 24 + face, RD, stride=24), :] = flux[v]


def finish_zones(acc, rf, fp, tb, polar, put, row_done):
    for k in range(RD):
        up, down = at(tb, 0, k), at(tb, 1, k)
        scale = polar[2:3, :] * at(tb, 2, k)
        for h in range(2):
            mine = slice(8 * h, 8 * h + 8)
            for v in range(NV):
                radial = rf[v, k + 1, mine, :] * up - rf[v, k, mine, :] * down
                azimuth = (fp[v, k, 8 * h + 1 : 8 * h + 9, :] - fp[v, k, mine, :]) * scale
                put(v, k, h, acc[v, k, mine, :] - radial - azimuth)
        if row_done is not None:
            row_done(k)


def kernel(
    x_ref, core_ref, polar_hbm, e0, acc, rf, fp, tb, polar, enc_v,
    e1, gt, rows_src, rows_in, l1_in, wedge_src, wedge_in, plane_src, plane_in,
    load_sem, h_send, h_recv, r_send, r_recv, a_send, a_recv, w_send, w_recv, b_send, b_recv, here_sem,
):
    r, y = lax.axis_index("radial"), lax.axis_index("phi")
    zc, xi = lax.rem(r, ZC), r // ZC
    first, last = r == 0, r == RADIAL - 1
    inner_there, outer_there = jnp.logical_not(first), jnp.logical_not(last)

    load = pltpu.make_async_copy(x_ref, e0.at[:, 2 : 2 + RD, PAD : PAD + NW, :], load_sem.at[0])
    polar_load = pltpu.make_async_copy(polar_hbm, polar, load_sem.at[1])
    load.start()
    polar_load.start()

    line = [(xi * ZC + lax.rem(zc + d, ZC), y) for d in range(1, ZC)]
    wedge = [(r, lax.rem(y + d, YN)) for d in range(1, YN)]
    barrier = pltpu.get_barrier_semaphore()

    def greet(device):
        pl.semaphore_signal(barrier, inc=1, device_id=device, device_id_type=MESH)

    across = [(lax.rem(xi + d, XN) * ZC + zc, y) for d in range(1, XN)]
    for device in line + wedge + across:
        greet(device)
    pl.when(inner_there)(lambda: greet((r - 1, y)))
    pl.when(outer_there)(lambda: greet((r + 1, y)))

    row = lax.broadcasted_iota(jnp.int32, (16, NT), 0)
    center = INNER_RADIUS + ((r * RD - 2 + row).astype(jnp.float32) + 0.5) * DR
    square = center * center
    below, above = center - 0.5 * DR, center + 0.5 * DR
    tb[0] = 0.5 * DT * (above * above) / (square * DR)
    tb[1] = 0.5 * DT * (below * below) / (square * DR)
    tb[2] = 1.0 / center
    tb[3] = (STRENGTH * DT) / square
    tb[4] = square

    polar_load.wait()
    load.wait()

    weight = polar[4:5, :]
    total = None
    for k in range(RD):
        part = e0[0, 2 + k, PAD : PAD + 8, :] + e0[0, 2 + k, PAD + 8 : PAD + 16, :]
        part = jnp.sum(part, axis=0, keepdims=True) * weight * at(tb, 4, k)
        rows_src[k : k + 1, :] = part
        total = part if total is None else total + part
    l1_in[pl.ds(zc, 1)] = total[None]

    count = ZC - 1 + YN - 1 + XN - 1 + jnp.where(first, 0, 1) + jnp.where(last, 0, 1)
    pl.semaphore_wait(barrier, count)

    def remote(src, dst, send, recv, device):
        return pltpu.make_async_remote_copy(
            src_ref=src, dst_ref=dst, send_sem=send, recv_sem=recv, device_id=device, device_id_type=MESH
        )

    def halo(e, base, which):
        phi_rows, own = pl.ds(2, RD), pl.ds(PAD, NW)
        src, dst, device = (
            (e.at[:, phi_rows, pl.ds(PAD, 2), :], e.at[:, phi_rows, pl.ds(PAD + NW, 2), :], (r, lax.rem(y + YN - 1, YN))),
            (e.at[:, phi_rows, pl.ds(PAD + NW - 2, 2), :], e.at[:, phi_rows, pl.ds(PAD - 2, 2), :], (r, lax.rem(y + 1, YN))),
            (e.at[:, pl.ds(2, 2), own, :], e.at[:, pl.ds(2 + RD, 2), own, :], (r - 1, y)),
            (e.at[:, pl.ds(RD, 2), own, :], e.at[:, pl.ds(0, 2), own, :], (r + 1, y)),
        )[which]
        return remote(src, dst, h_send.at[base + which], h_recv.at[base + which], device)

    def start_halos(e, base):
        pl.when(inner_there)(lambda: halo(e, base, 2).start())
        pl.when(outer_there)(lambda: halo(e, base, 3).start())
        halo(e, base, 0).start()
        halo(e, base, 1).start()

    def wait_halos(e, base):
        pl.when(outer_there)(lambda: halo(e, base, 2).wait_recv())
        pl.when(inner_there)(lambda: halo(e, base, 3).wait_recv())
        halo(e, base, 0).wait_recv()
        halo(e, base, 1).wait_recv()

    def wait_sent(e, base):
        pl.when(inner_there)(lambda: halo(e, base, 2).wait_send())
        pl.when(outer_there)(lambda: halo(e, base, 3).wait_send())
        halo(e, base, 0).wait_send()
        halo(e, base, 1).wait_send()

    def line_copy(d):
        return remote(l1_in.at[zc], l1_in.at[zc], a_send.at[d], a_recv.at[zc], line[d - 1])

    def line_sum(begin, end, start):
        def add(j, so_far):
            remote(l1_in.at[j], l1_in.at[j], a_send.at[0], a_recv.at[j], line[0]).wait_recv()
            return so_far + l1_in[j]

        return lax.fori_loop(begin, end, add, start)

    def rows_copy(group, device):
        return remote(rows_src, rows_in.at[group], r_send.at[group], r_recv.at[group], device)

    for d in range(1, ZC):
        line_copy(d).start()
    for d in range(1, XN):
        pl.when(xi - d >= 0)(
            lambda d=d: pl.semaphore_signal(here_sem, inc=1, device_id=(r - d * ZC, y), device_id_type=MESH)
        )
    start_halos(e0, 0)
    pl.when(inner_there)(lambda: rows_copy(1, (r - 1, y)).start())
    pl.when(outer_there)(lambda: rows_copy(0, (r + 1, y)).start())

    def edges(e):
        @pl.when(first)
        def _():
            for j in range(2):
                e[:, j, PAD : PAD + NW, :] = e[:, 2, PAD : PAD + NW, :]

        @pl.when(last)
        def _():
            for j in range(2):
                e[:, 2 + RD + j, PAD : PAD + NW, :] = e[:, 1 + RD, PAD : PAD + NW, :]

    polar_phase(e0, acc, tb, polar, None)
    radial_faces(e0, rf, ((2, RD - 1),))
    azimuth_inner(e0, fp)

    inner = line_sum(0, zc, jnp.zeros((1, NT), jnp.float32))
    pl.when(inner_there)(lambda: rows_copy(0, (r - 1, y)).wait_recv())
    pl.when(outer_there)(lambda: rows_copy(1, (r + 1, y)).wait_recv())

    @pl.when(first)
    def _():
        rows_in[0] = jnp.zeros((RD, NT), jnp.float32)

    @pl.when(last)
    def _():
        rows_in[1] = jnp.zeros((RD, NT), jnp.float32)

    wedge_src[0:RD, :] = rows_src[...]
    wedge_src[8:9, :] = inner
    wedge_src[9:11, :] = rows_in[0, RD - 2 : RD, :]
    wedge_src[11:13, :] = rows_in[1, 0:2, :]
    wedge_src[13:16, :] = jnp.zeros((3, NT), jnp.float32)

    def wedge_copy(d, slot):
        return remote(wedge_src, wedge_in.at[slot], w_send.at[d], w_recv.at[slot], wedge[d - 1])

    def plane_copy(sem, slot, device):
        return remote(plane_src, plane_in.at[slot], b_send.at[sem], b_recv.at[slot], device)

    for d in range(1, YN):
        wedge_copy(d, y).start()
    plane_src[...] = line_sum(zc + 1, ZC, inner + total)
    pl.when(xi < XN - 1)(lambda: pl.semaphore_wait(here_sem, XN - 1 - xi))

    def each_wedge(act):
        for yy in range(YN):
            act(yy)

    me = xi * YN + y
    for d in range(1, XN):
        pl.when(xi + d < XN)(
            lambda d=d: each_wedge(lambda yy: plane_copy(d * YN + yy, me, (r + d * ZC, yy)).start())
        )

    wait_halos(e0, 0)
    edges(e0)
    radial_faces(e0, rf, ((0, 2), (RD - 1, RD + 1)))
    azimuth_outer(e0, fp)

    def put(v, k, h, value):
        e1[v, k + 2, PAD + 8 * h : PAD + 8 * h + 8, :] = value

    finish_zones(acc, rf, fp, tb, polar, put, None)
    start_halos(e1, 4)

    parts = wedge_src[...]
    for d in range(1, YN):
        j = lax.rem(y + d, YN)
        wedge_copy(d, j).wait_recv()
        parts = parts + wedge_in[j]

    def plane_sum(j, so_far):
        plane_copy(0, j, wedge[0]).wait_recv()
        return so_far + plane_in[j]

    base = lax.fori_loop(0, xi * YN, plane_sum, parts[8:9, :])
    own, inside, outside = parts[0:RD, :], parts[9:11, :], parts[11:13, :]
    one = [own[k : k + 1, :] for k in range(RD)]
    gt[1:2, :] = base - 0.5 * inside[1:2, :]
    gt[0:1, :] = base - inside[1:2, :] - 0.5 * inside[0:1, :]
    sofar = base
    for k in range(RD):
        gt[k + 2 : k + 3, :] = sofar + 0.5 * one[k]
        sofar = sofar + one[k]
    gt[RD + 2 : RD + 3, :] = sofar + 0.5 * outside[0:1, :]
    gt[RD + 3 : RD + 4, :] = sofar + outside[0:1, :] + 0.5 * outside[1:2, :]
    gt[RD + 4 : 16, :] = jnp.zeros((4, NT), jnp.float32)
    enclosed = jnp.broadcast_to(jnp.sum(gt[...], axis=1, keepdims=True), (16, NT)) + core_ref[0]
    diagonal = lax.broadcasted_iota(jnp.int32, (16, NT), 1) + 2 == row
    enc_v[...] = jnp.sum(jnp.where(diagonal, enclosed, 0.0), axis=0, keepdims=True)
    gt[...] = enclosed * tb[3]

    def pull_down(k, rows):
        pull = gt[pl.ds(k + 2, 1), :]
        density = jnp.maximum(e0[0, k + 2, rows, :], MINIMUM_DENSITY)
        e1[1, k + 2, rows, :] = e1[1, k + 2, rows, :] - density * pull
        e1[4, k + 2, rows, :] = e1[4, k + 2, rows, :] - e0[1, k + 2, rows, :] * pull

    wait_sent(e1, 4)
    for k in range(RD):
        pull_down(k, pl.ds(PAD, NW))

    polar_phase(e1, acc, tb, polar, gt)
    radial_faces(e1, rf, ((2, RD - 1),))
    azimuth_inner(e1, fp)
    wait_halos(e1, 4)
    for k in range(RD):
        pull_down(k, pl.ds(PAD - 2, 2))
        pull_down(k, pl.ds(PAD + NW, 2))
    for k in (-2, -1, RD, RD + 1):
        pull_down(k, pl.ds(PAD, NW))
    edges(e1)
    radial_faces(e1, rf, ((0, 2), (RD - 1, RD + 1)))
    azimuth_outer(e1, fp)

    wait_sent(e0, 0)
    for d in range(1, ZC):
        line_copy(d).wait_send()
    for d in range(1, YN):
        wedge_copy(d, y).wait_send()
    pl.when(inner_there)(lambda: rows_copy(1, (r - 1, y)).wait_send())
    pl.when(outer_there)(lambda: rows_copy(0, (r + 1, y)).wait_send())
    for d in range(1, XN):
        pl.when(xi + d < XN)(
            lambda d=d: each_wedge(lambda yy: plane_copy(d * YN + yy, me, (r + d * ZC, yy)).wait_send())
        )


def last_kernel(e0, acc, rf, fp, tb, polar, enc_v, out_ref, enc_ref, out_v, sem):
    enc_ref[...] = enc_v[0, :][:RD]

    def put(v, k, h, value):
        out_v[v, k, 8 * h : 8 * h + 8, :] = 0.5 * (e0[v, k + 2, PAD + 8 * h : PAD + 8 * h + 8, :] + value)

    def store(k):
        return pltpu.make_async_copy(out_v.at[:, k], out_ref.at[:, k], sem.at[k])

    finish_zones(acc, rf, fp, tb, polar, put, lambda k: store(k).start())
    for k in range(RD):
        store(k).wait()


def body(conserved, core_mass):
    f32 = jnp.float32
    dma = pltpu.SemaphoreType.DMA
    vmem, anywhere = pltpu.VMEM, pl.BlockSpec(memory_space=pl.ANY)
    resident = pl.BlockSpec(memory_space=vmem)
    polar = pltpu.with_memory_space_constraint(jnp.asarray(polar_table()), pltpu.HBM)
    conserved = pltpu.with_memory_space_constraint(conserved, pltpu.HBM)
    extended = vmem((NV, RD + 4, ROWS, NT), f32)
    slab = vmem((NV, RD, NW, NT), f32)
    radial_flux, azimuth_fluxes = vmem((NV, RD + 1, NW, NT), f32), vmem((NV, RD, 24, NT), f32)
    held = pl.pallas_call(
        kernel,
        out_shape=(
            extended, slab, radial_flux, azimuth_fluxes, vmem((5, 16, NT), f32), vmem((8, NT), f32), vmem((1, NT), f32),
        ),
        in_specs=[anywhere, pl.BlockSpec(memory_space=pltpu.SMEM), anywhere],
        out_specs=(resident,) * 7,
        scratch_shapes=[
            extended, vmem((16, NT), f32),
            vmem((RD, NT), f32), vmem((2, RD, NT), f32), vmem((ZC, 1, NT), f32),
            vmem((16, NT), f32), vmem((YN, 16, NT), f32), vmem((1, NT), f32), vmem((XN * YN, 1, NT), f32),
            dma((2,)), dma((8,)), dma((8,)), dma((2,)), dma((2,)), dma((ZC,)), dma((ZC,)),
            dma((YN,)), dma((YN,)), dma((XN * YN,)), dma((XN * YN,)), pltpu.SemaphoreType.REGULAR,
        ],
        compiler_params=pltpu.CompilerParams(
            collective_id=0, has_side_effects=True, vmem_limit_bytes=VMEM_LIMIT
        ),
        name="two_sections",
    )(conserved, core_mass, polar)
    e0, acc, rf, fp, tb, polar, enc_v = (pltpu.with_memory_space_constraint(a, vmem) for a in held)
    return pl.pallas_call(
        last_kernel,
        out_shape=(jax.ShapeDtypeStruct(conserved.shape, f32), jax.ShapeDtypeStruct((RD,), f32)),
        in_specs=[resident] * 7,
        out_specs=(anywhere, resident),
        scratch_shapes=[slab, dma((RD,))],
        compiler_params=pltpu.CompilerParams(vmem_limit_bytes=VMEM_LIMIT),
        name="last_faces",
    )(e0, acc, rf, fp, tb, polar, enc_v)


def solution(mesh):
    in_specs = (P(None, "radial", "phi", None), P())
    out_specs = (P(None, "radial", "phi", None), P("radial"))
    return jax.shard_map(body, mesh=mesh, in_specs=in_specs, out_specs=out_specs, check_vma=False)
```

```python
import math

import jax
import jax.numpy as jnp
import numpy as np
from jax import lax
from jax.experimental import pallas as pl
from jax.experimental.pallas import tpu as pltpu
from jax.sharding import PartitionSpec as P

ADIABATIC = 4.0 / 3.0
INNER_RADIUS = 1.0
OUTER_RADIUS = 2.0
COURANT = 0.4
GRAVITY_KICK = 0.004
MINIMUM_DENSITY = 0.05
PRESSURE_FLOOR = 0.01

MESH = pl.DeviceIdType.MESH
NV = 8
RD = 8
NW = 16
NT = 128
PAD = 8
ROWS = 40
XN, ZC, YN = 4, 16, 4
RADIAL = XN * ZC
VMEM_LIMIT = 24 << 20


def step_sizes(radial_total, phi_total, theta_total):
    theta_step = math.pi / theta_total
    phi_step = 2.0 * math.pi / phi_total
    polar_width = INNER_RADIUS * math.sin(0.5 * theta_step) * phi_step
    radial_step = min(2.0 * polar_width, (OUTER_RADIUS - INNER_RADIUS) / radial_total)
    timestep = COURANT * min(radial_step, polar_width)
    return (radial_step, theta_step, phi_step, timestep)


DR, DTH, DPH, DT = step_sizes(RADIAL * RD, YN * NW, NT)
STRENGTH = GRAVITY_KICK / DT


def polar_table():
    center = (np.arange(NT) + 0.5) * DTH
    face = np.arange(NT + 1) * DTH
    sine, face_sine = np.sin(center), np.sin(face)
    table = np.zeros((8, NT))
    table[0] = 0.5 * DT * face_sine[:-1] / (sine * DTH)
    table[1] = 0.5 * DT * face_sine[1:] / (sine * DTH)
    table[2] = 0.5 * DT / (sine * DPH)
    table[3] = np.cos(center) / sine
    table[4] = sine * (DR * DTH * DPH)
    return table.astype(np.float32)


def thermo(u):
    density = jnp.maximum(u[0], MINIMUM_DENSITY)
    inverse = 1.0 / density
    kinetic = 0.5 * (u[1] * u[1] + u[2] * u[2] + u[3] * u[3]) * inverse
    pressure = jnp.maximum((ADIABATIC - 1.0) * (u[4] - kinetic), PRESSURE_FLOOR * density)
    return density, inverse, pressure


def side(u, m):
    _, inverse, pressure = thermo(u)
    normal = u[m] * inverse
    square = ADIABATIC * pressure * inverse
    return pressure, normal, jnp.abs(normal) + square * lax.rsqrt(square)


def minmod(a, b):
    return jnp.maximum(jnp.minimum(a, b), jnp.minimum(jnp.maximum(a, b), 0.0))


def twice_flux(left, right, m):
    pl_, vl, al = side(left, m)
    pr_, vr, ar = side(right, m)
    signal = jnp.maximum(al, ar)
    cl, cr = vl + signal, vr - signal
    flux = [cl * a + cr * b for a, b in zip(left, right)]
    flux[m] = flux[m] + (pl_ + pr_)
    flux[4] = flux[4] + (pl_ * vl + pr_ * vr)
    return flux


def at(tb, table, k):
    return tb[table, pl.ds(k + 2, 1), :]


def polar_phase(e, acc, tb, polar, gt):
    is_first_lane = lax.broadcasted_iota(jnp.int32, (8, NT), 1) == 0

    def tile(k, h):
        u = [e[v, k + 2, PAD + 8 * h : PAD + 8 * h + 8, :] for v in range(NV)]
        left, right = [], []
        for v in range(NV):
            back = pltpu.roll(u[v], 1, 1)
            diff = jnp.where(is_first_lane, 0.0, u[v] - back)
            slope = 0.5 * minmod(diff, pltpu.roll(diff, NT - 1, 1))
            left.append(pltpu.roll(u[v] + slope, 1, 1))
            right.append(jnp.where(is_first_lane, back, u[v] - slope))
        flux = twice_flux(left, right, 2)
        inverse_r = at(tb, 2, k)
        low, high = polar[0:1, :] * inverse_r, polar[1:2, :] * inverse_r
        new = [u[v] - (pltpu.roll(flux[v], NT - 1, 1) * high - flux[v] * low) for v in range(NV)]
        density, inverse, pressure = thermo(u)
        v1, v2, v3 = u[1] * inverse, u[2] * inverse, u[3] * inverse
        cot, step_r = polar[3:4, :], DT * inverse_r
        d3 = density * v3
        d33 = d3 * v3
        new[1] = new[1] + (2.0 * pressure + density * (v2 * v2) + d33) * step_r
        new[2] = new[2] + ((pressure + d33) * cot - density * v1 * v2) * step_r
        new[3] = new[3] - d3 * (v1 + v2 * cot) * step_r
        if gt is not None:
            pull = gt[pl.ds(k + 2, 1), :]
            new[1] = new[1] - density * pull
            new[4] = new[4] - u[1] * pull
        for v in range(NV):
            acc[v, k, 8 * h : 8 * h + 8, :] = new[v]

    def step(k, _):
        for h in range(2):
            tile(k, h)
        return 0

    lax.fori_loop(0, RD, step, 0, unroll=4)


def radial_faces(e, rf, spans):
    def step(h, _):
        rows = pl.ds(pl.multiple_of(PAD + 8 * h, 8), 8)
        mine = pl.ds(pl.multiple_of(8 * h, 8), 8)
        for begin, end in spans:
            value = [e[v, begin + 1, rows, :] for v in range(NV)]
            diff = [value[v] - e[v, begin, rows, :] for v in range(NV)]
            left = None
            for k in range(begin - 1, end):
                after = [e[v, k + 3, rows, :] for v in range(NV)]
                ahead = [after[v] - value[v] for v in range(NV)]
                slope = [0.5 * minmod(diff[v], ahead[v]) for v in range(NV)]
                if k >= begin:
                    flux = twice_flux(left, [value[v] - slope[v] for v in range(NV)], 1)
                    for v in range(NV):
                        rf[v, k, mine, :] = flux[v]
                left = [value[v] + slope[v] for v in range(NV)]
                value, diff = after, ahead
        return 0

    lax.fori_loop(0, 2, step, 0)


def azimuth_flux(load_at):
    u = [[load_at(v, s) for v in range(NV)] for s in range(-2, 2)]
    back = [u[1][v] - u[0][v] for v in range(NV)]
    here = [u[2][v] - u[1][v] for v in range(NV)]
    ahead = [u[3][v] - u[2][v] for v in range(NV)]
    left = [u[1][v] + 0.5 * minmod(back[v], here[v]) for v in range(NV)]
    right = [u[2][v] - 0.5 * minmod(here[v], ahead[v]) for v in range(NV)]
    return twice_flux(left, right, 3)


def azimuth_inner(e, fp):
    def step(k, _):
        for face in (2, 7):
            flux = azimuth_flux(lambda v, s: e[v, k + 2, PAD + face + s : PAD + face + s + 8, :])
            for v in range(NV):
                fp[v, k, face : face + 8, :] = flux[v]
        return 0

    lax.fori_loop(0, RD, step, 0)


def azimuth_outer(e, fp):
    flat = e.reshape(NV * 12 * ROWS, NT)
    fp_flat = fp.reshape(NV * RD * 24, NT)
    for face in (0, 1, NW - 1, NW):
        flux = azimuth_flux(
            lambda v, s: flat[pl.ds((v * 12 + 2) * ROWS + PAD + face + s, RD, stride=ROWS), :]
        )
        for v in range(NV):
            fp_flat[pl.ds(v * RD * 24 + face, RD, stride=24), :] = flux[v]


def finish_zones(acc, rf, fp, tb, polar, put, row_done):
    for k in range(RD):
        up, down = at(tb, 0, k), at(tb, 1, k)
        scale = polar[2:3, :] * at(tb, 2, k)
        for h in range(2):
            mine = slice(8 * h, 8 * h + 8)
            for v in range(NV):
                radial = rf[v, k + 1, mine, :] * up - rf[v, k, mine, :] * down
                azimuth = (fp[v, k, 8 * h + 1 : 8 * h + 9, :] - fp[v, k, mine, :]) * scale
                put(v, k, h, acc[v, k, mine, :] - radial - azimuth)
        if row_done is not None:
            row_done(k)


def kernel(
    x_ref, core_ref, polar_hbm, e0, acc, rf, fp, tb, polar, enc_v,
    e1, gt, rows_src, rows_in, l1_in, wedge_src, wedge_in, plane_src, plane_in,
    load_sem, h_send, h_recv, r_send, r_recv, a_send, a_recv, w_send, w_recv, b_send, b_recv, here_sem,
):
    r, y = lax.axis_index("radial"), lax.axis_index("phi")
    zc, xi = lax.rem(r, ZC), r // ZC
    first, last = r == 0, r == RADIAL - 1
    inner_there, outer_there = jnp.logical_not(first), jnp.logical_not(last)

    load = pltpu.make_async_copy(x_ref, e0.at[:, 2 : 2 + RD, PAD : PAD + NW, :], load_sem.at[0])
    polar_load = pltpu.make_async_copy(polar_hbm, polar, load_sem.at[1])
    load.start()
    polar_load.start()

    line = [(xi * ZC + lax.rem(zc + d, ZC), y) for d in range(1, ZC)]
    wedge = [(r, lax.rem(y + d, YN)) for d in range(1, YN)]
    barrier = pltpu.get_barrier_semaphore()

    def greet(device):
        pl.semaphore_signal(barrier, inc=1, device_id=device, device_id_type=MESH)

    across = [(lax.rem(xi + d, XN) * ZC + zc, y) for d in range(1, XN)]
    for device in line + wedge + across:
        greet(device)
    pl.when(inner_there)(lambda: greet((r - 1, y)))
    pl.when(outer_there)(lambda: greet((r + 1, y)))

    row = lax.broadcasted_iota(jnp.int32, (16, NT), 0)
    center = INNER_RADIUS + ((r * RD - 2 + row).astype(jnp.float32) + 0.5) * DR
    square = center * center
    below, above = center - 0.5 * DR, center + 0.5 * DR
    tb[0] = 0.5 * DT * (above * above) / (square * DR)
    tb[1] = 0.5 * DT * (below * below) / (square * DR)
    tb[2] = 1.0 / center
    tb[3] = (STRENGTH * DT) / square
    tb[4] = square

    polar_load.wait()
    load.wait()

    weight = polar[4:5, :]
    total = None
    for k in range(RD):
        part = e0[0, 2 + k, PAD : PAD + 8, :] + e0[0, 2 + k, PAD + 8 : PAD + 16, :]
        part = jnp.sum(part, axis=0, keepdims=True) * weight * at(tb, 4, k)
        rows_src[k : k + 1, :] = part
        total = part if total is None else total + part
    l1_in[pl.ds(zc, 1)] = total[None]

    count = ZC - 1 + YN - 1 + XN - 1 + jnp.where(first, 0, 1) + jnp.where(last, 0, 1)
    pl.semaphore_wait(barrier, count)

    def remote(src, dst, send, recv, device):
        return pltpu.make_async_remote_copy(
            src_ref=src, dst_ref=dst, send_sem=send, recv_sem=recv, device_id=device, device_id_type=MESH
        )

    def halo(e, base, which):
        phi_rows, own = pl.ds(2, RD), pl.ds(PAD, NW)
        src, dst, device = (
            (e.at[:, phi_rows, pl.ds(PAD, 2), :], e.at[:, phi_rows, pl.ds(PAD + NW, 2), :], (r, lax.rem(y + YN - 1, YN))),
            (e.at[:, phi_rows, pl.ds(PAD + NW - 2, 2), :], e.at[:, phi_rows, pl.ds(PAD - 2, 2), :], (r, lax.rem(y + 1, YN))),
            (e.at[:, pl.ds(2, 2), own, :], e.at[:, pl.ds(2 + RD, 2), own, :], (r - 1, y)),
            (e.at[:, pl.ds(RD, 2), own, :], e.at[:, pl.ds(0, 2), own, :], (r + 1, y)),
        )[which]
        return remote(src, dst, h_send.at[base + which], h_recv.at[base + which], device)

    def start_halos(e, base):
        pl.when(inner_there)(lambda: halo(e, base, 2).start())
        pl.when(outer_there)(lambda: halo(e, base, 3).start())
        halo(e, base, 0).start()
        halo(e, base, 1).start()

    def wait_halos(e, base):
        pl.when(outer_there)(lambda: halo(e, base, 2).wait_recv())
        pl.when(inner_there)(lambda: halo(e, base, 3).wait_recv())
        halo(e, base, 0).wait_recv()
        halo(e, base, 1).wait_recv()

    def wait_sent(e, base):
        pl.when(inner_there)(lambda: halo(e, base, 2).wait_send())
        pl.when(outer_there)(lambda: halo(e, base, 3).wait_send())
        halo(e, base, 0).wait_send()
        halo(e, base, 1).wait_send()

    def line_copy(d):
        return remote(l1_in.at[zc], l1_in.at[zc], a_send.at[d], a_recv.at[zc], line[d - 1])

    def line_sum(begin, end, start):
        def add(j, so_far):
            remote(l1_in.at[j], l1_in.at[j], a_send.at[0], a_recv.at[j], line[0]).wait_recv()
            return so_far + l1_in[j]

        return lax.fori_loop(begin, end, add, start)

    def rows_copy(group, device):
        return remote(rows_src, rows_in.at[group], r_send.at[group], r_recv.at[group], device)

    for d in range(1, ZC):
        line_copy(d).start()
    for d in range(1, XN):
        pl.when(xi - d >= 0)(
            lambda d=d: pl.semaphore_signal(here_sem, inc=1, device_id=(r - d * ZC, y), device_id_type=MESH)
        )
    start_halos(e0, 0)
    pl.when(inner_there)(lambda: rows_copy(1, (r - 1, y)).start())
    pl.when(outer_there)(lambda: rows_copy(0, (r + 1, y)).start())

    def edges(e):
        @pl.when(first)
        def _():
            for j in range(2):
                e[:, j, PAD : PAD + NW, :] = e[:, 2, PAD : PAD + NW, :]

        @pl.when(last)
        def _():
            for j in range(2):
                e[:, 2 + RD + j, PAD : PAD + NW, :] = e[:, 1 + RD, PAD : PAD + NW, :]

    polar_phase(e0, acc, tb, polar, None)
    radial_faces(e0, rf, ((2, RD - 1),))
    azimuth_inner(e0, fp)

    inner = line_sum(0, zc, jnp.zeros((1, NT), jnp.float32))
    pl.when(inner_there)(lambda: rows_copy(0, (r - 1, y)).wait_recv())
    pl.when(outer_there)(lambda: rows_copy(1, (r + 1, y)).wait_recv())

    @pl.when(first)
    def _():
        rows_in[0] = jnp.zeros((RD, NT), jnp.float32)

    @pl.when(last)
    def _():
        rows_in[1] = jnp.zeros((RD, NT), jnp.float32)

    wedge_src[0:RD, :] = rows_src[...]
    wedge_src[8:9, :] = inner
    wedge_src[9:11, :] = rows_in[0, RD - 2 : RD, :]
    wedge_src[11:13, :] = rows_in[1, 0:2, :]
    wedge_src[13:16, :] = jnp.zeros((3, NT), jnp.float32)

    def wedge_copy(d, slot):
        return remote(wedge_src, wedge_in.at[slot], w_send.at[d], w_recv.at[slot], wedge[d - 1])

    def plane_copy(sem, slot, device):
        return remote(plane_src, plane_in.at[slot], b_send.at[sem], b_recv.at[slot], device)

    for d in range(1, YN):
        wedge_copy(d, y).start()
    plane_src[...] = line_sum(zc + 1, ZC, inner + total)
    pl.when(xi < XN - 1)(lambda: pl.semaphore_wait(here_sem, XN - 1 - xi))

    def each_wedge(act):
        for yy in range(YN):
            act(yy)

    me = xi * YN + y
    for d in range(1, XN):
        pl.when(xi + d < XN)(
            lambda d=d: each_wedge(lambda yy: plane_copy(d * YN + yy, me, (r + d * ZC, yy)).start())
        )

    wait_halos(e0, 0)
    edges(e0)
    radial_faces(e0, rf, ((0, 2), (RD - 1, RD + 1)))
    azimuth_outer(e0, fp)

    def put(v, k, h, value):
        e1[v, k + 2, PAD + 8 * h : PAD + 8 * h + 8, :] = value

    finish_zones(acc, rf, fp, tb, polar, put, None)
    start_halos(e1, 4)

    parts = wedge_src[...]
    for d in range(1, YN):
        j = lax.rem(y + d, YN)
        wedge_copy(d, j).wait_recv()
        parts = parts + wedge_in[j]

    def plane_sum(j, so_far):
        plane_copy(0, j, wedge[0]).wait_recv()
        return so_far + plane_in[j]

    base = lax.fori_loop(0, xi * YN, plane_sum, parts[8:9, :])
    own, inside, outside = parts[0:RD, :], parts[9:11, :], parts[11:13, :]
    one = [own[k : k + 1, :] for k in range(RD)]
    gt[1:2, :] = base - 0.5 * inside[1:2, :]
    gt[0:1, :] = base - inside[1:2, :] - 0.5 * inside[0:1, :]
    sofar = base
    for k in range(RD):
        gt[k + 2 : k + 3, :] = sofar + 0.5 * one[k]
        sofar = sofar + one[k]
    gt[RD + 2 : RD + 3, :] = sofar + 0.5 * outside[0:1, :]
    gt[RD + 3 : RD + 4, :] = sofar + outside[0:1, :] + 0.5 * outside[1:2, :]
    gt[RD + 4 : 16, :] = jnp.zeros((4, NT), jnp.float32)
    enclosed = jnp.broadcast_to(jnp.sum(gt[...], axis=1, keepdims=True), (16, NT)) + core_ref[0]
    diagonal = lax.broadcasted_iota(jnp.int32, (16, NT), 1) + 2 == row
    enc_v[...] = jnp.sum(jnp.where(diagonal, enclosed, 0.0), axis=0)[:RD]
    gt[...] = enclosed * tb[3]

    def pull_down(k, rows):
        pull = gt[pl.ds(k + 2, 1), :]
        density = jnp.maximum(e0[0, k + 2, rows, :], MINIMUM_DENSITY)
        e1[1, k + 2, rows, :] = e1[1, k + 2, rows, :] - density * pull
        e1[4, k + 2, rows, :] = e1[4, k + 2, rows, :] - e0[1, k + 2, rows, :] * pull

    wait_sent(e1, 4)
    for k in range(RD):
        pull_down(k, pl.ds(PAD, NW))

    polar_phase(e1, acc, tb, polar, gt)
    radial_faces(e1, rf, ((2, RD - 1),))
    azimuth_inner(e1, fp)
    wait_halos(e1, 4)
    for k in range(RD):
        pull_down(k, pl.ds(PAD - 2, 2))
        pull_down(k, pl.ds(PAD + NW, 2))
    for k in (-2, -1, RD, RD + 1):
        pull_down(k, pl.ds(PAD, NW))
    edges(e1)
    radial_faces(e1, rf, ((0, 2), (RD - 1, RD + 1)))
    azimuth_outer(e1, fp)

    wait_sent(e0, 0)
    for d in range(1, ZC):
        line_copy(d).wait_send()
    for d in range(1, YN):
        wedge_copy(d, y).wait_send()
    pl.when(inner_there)(lambda: rows_copy(1, (r - 1, y)).wait_send())
    pl.when(outer_there)(lambda: rows_copy(0, (r + 1, y)).wait_send())
    for d in range(1, XN):
        pl.when(xi + d < XN)(
            lambda d=d: each_wedge(lambda yy: plane_copy(d * YN + yy, me, (r + d * ZC, yy)).wait_send())
        )


def last_kernel(e0, acc, rf, fp, tb, polar, enc_v, out_ref, enc_ref, out_v, sem):
    enc_store = pltpu.make_async_copy(enc_v, enc_ref, sem.at[RD])
    enc_store.start()

    def put(v, k, h, value):
        out_v[v, k, 8 * h : 8 * h + 8, :] = 0.5 * (e0[v, k + 2, PAD + 8 * h : PAD + 8 * h + 8, :] + value)

    def store(k):
        return pltpu.make_async_copy(out_v.at[:, k], out_ref.at[:, k], sem.at[k])

    finish_zones(acc, rf, fp, tb, polar, put, lambda k: store(k).start())
    for k in range(RD):
        store(k).wait()
    enc_store.wait()


def body(conserved, core_mass):
    f32 = jnp.float32
    dma = pltpu.SemaphoreType.DMA
    vmem, anywhere = pltpu.VMEM, pl.BlockSpec(memory_space=pl.ANY)
    resident = pl.BlockSpec(memory_space=vmem)
    polar = pltpu.with_memory_space_constraint(jnp.asarray(polar_table()), pltpu.HBM)
    conserved = pltpu.with_memory_space_constraint(conserved, pltpu.HBM)
    extended = vmem((NV, RD + 4, ROWS, NT), f32)
    slab = vmem((NV, RD, NW, NT), f32)
    radial_flux, azimuth_fluxes = vmem((NV, RD + 1, NW, NT), f32), vmem((NV, RD, 24, NT), f32)
    held = pl.pallas_call(
        kernel,
        out_shape=(
            extended, slab, radial_flux, azimuth_fluxes, vmem((5, 16, NT), f32), vmem((8, NT), f32), vmem((RD,), f32),
        ),
        in_specs=[anywhere, pl.BlockSpec(memory_space=pltpu.SMEM), anywhere],
        out_specs=(resident,) * 7,
        scratch_shapes=[
            extended, vmem((16, NT), f32),
            vmem((RD, NT), f32), vmem((2, RD, NT), f32), vmem((ZC, 1, NT), f32),
            vmem((16, NT), f32), vmem((YN, 16, NT), f32), vmem((1, NT), f32), vmem((XN * YN, 1, NT), f32),
            dma((2,)), dma((8,)), dma((8,)), dma((2,)), dma((2,)), dma((ZC,)), dma((ZC,)),
            dma((YN,)), dma((YN,)), dma((XN * YN,)), dma((XN * YN,)), pltpu.SemaphoreType.REGULAR,
        ],
        compiler_params=pltpu.CompilerParams(
            collective_id=0, has_side_effects=True, vmem_limit_bytes=VMEM_LIMIT
        ),
        name="two_sections",
    )(conserved, core_mass, polar)
    e0, acc, rf, fp, tb, polar, enc_v = (pltpu.with_memory_space_constraint(a, vmem) for a in held)
    return pl.pallas_call(
        last_kernel,
        out_shape=(jax.ShapeDtypeStruct(conserved.shape, f32), jax.ShapeDtypeStruct((RD,), f32)),
        in_specs=[resident] * 7,
        out_specs=(anywhere, anywhere),
        scratch_shapes=[slab, dma((RD + 1,))],
        compiler_params=pltpu.CompilerParams(vmem_limit_bytes=VMEM_LIMIT),
        name="last_faces",
    )(e0, acc, rf, fp, tb, polar, enc_v)


def solution(mesh):
    in_specs = (P(None, "radial", "phi", None), P())
    out_specs = (P(None, "radial", "phi", None), P("radial"))
    return jax.shard_map(body, mesh=mesh, in_specs=in_specs, out_specs=out_specs, check_vma=False)
```
